32 devices in a mesh: tm: 8 (over z, y), col: 4 (over x, core).
Axes of the slice: x: 2, y: 2, z: 4, core: 2. Of those that a mesh axis runs over, the one named last changes fastest.
Arguments:
- block_values: bfloat16 [4, 16384, 128], P('col', 'tm'), may hold values from -6 to 6
- block_shifts: bfloat16 [4, 16384, 128], P('col', 'tm'), may hold values from -1 to 1
- block_sensor: int32 [4, 16384], P('col', 'tm'), may hold values from 0 to 4095
- block_window: int32 [4, 16384], P('col', 'tm'), may hold values from 0 to 3
- block_owner: int32 [4, 16384, 1], P('col', 'tm'), may hold values from 0 to 7; in each aligned block of 2048 rows (0 to 2047, 2048 to 4095, ..., all dimensions but the last counted through in order) at most 384 rows name the same one
- block_counts: int32 [4, 8], P('col', 'tm'), may hold values from 1536 to 2048
- calibration: bfloat16 [16384, 4096], P('tm', 'col'), may hold values from -0.046875 to 0.046875
Outputs:
- calibrated: bfloat16 [4096, 4096], P('tm', 'col')
The draws below stay inside these ranges and needn't reach their ends.
Inputs may be any that keep to these rules, and one draw needn't show every extreme that they name: `block_owner`: among the 2048 block slots of one device, at most 384 name the same owner, a bound that some block reaches. The live blocks of device (tm t, col c) are its first block_counts[c, t] slots.
All inputs are finite; a program needn't handle non-finite values.
Results may differ from the reference program's by a relative error of at most 0.015.
Values may be sent and summed in bfloat16 or wider, within the bound.
A program may use at most 128 MiB of HBM per device.

```python
import math
import jax
import jax.numpy as jnp
import numpy as np
from jax import lax

SENSORS = 16384
OUTPUTS = 4096
BLOCK_LEN = 128
BLOCKS_DEV = 2048
WINDOWS = 4
CAPACITY = 384
GROUP_SENSORS = 4096
BLOCK_ROWS = 16384
GRID_ROWS = 4096
N_TM = 8
N_COL = 4


def plant(drawn, key, low, high):
    extent = drawn.shape
    index_at = [jax.random.randint(jax.random.fold_in(key, axis), (), 0, extent[axis]) for axis in range(len(extent))]
    drawn = drawn.at[tuple(index_at)].set(low)
    longest = extent.index(max(extent))
    index_at[longest] = (index_at[longest] + 1) % extent[longest]
    return drawn.at[tuple(index_at)].set(high)


def steps_of(key, dims, shards, low, top_value):
    level, own = 1.0, jax.random.fold_in(key, 6)
    for dim, blocks in shards:
        draws = jnp.exp(jax.random.uniform(jax.random.fold_in(own, dim), (blocks,), jnp.float32, low / len(shards), top_value / len(shards)))
        level = level * jnp.repeat(draws, dims[dim] // blocks).reshape([-1 if axis == dim else 1 for axis in range(len(dims))])
    return level


def deal_out(stream_key, own, number, rows, count, top, reach, slope):
    sequence = jax.random.permutation(stream_key, count)
    packed, usual = load_shares(count, rows * top, reach, slope, True), load_shares(count, rows * top, reach, slope, False)
    places = jnp.arange(count)

    def named(lengths, offset_by):
        used = int((lengths > 0).sum())
        fixed = max(1, used // 4)
        shifted = fixed + (places - fixed + offset_by * (used - fixed)) % max(1, count - fixed)
        return jnp.zeros((count,), jnp.int32).at[sequence[jnp.where(places < fixed, places, shifted)]].set(jnp.asarray(lengths, jnp.int32))

    lengths = jnp.where(number % 4 == 0, named(packed, number // 4), named(usual, number - number // 4 - 1))
    mixed = jax.random.permutation(jax.random.fold_in(own, 3), count)
    donor, sink = mixed[0:count // 2 * 2:2], mixed[1:count // 2 * 2:2]
    margin = jnp.minimum(lengths[donor] - 1, reach - lengths[sink]) // 2
    margin = jnp.where((donor == sequence[0]) | (sink == sequence[0]) | (lengths[sink] == 0), 0, jnp.maximum(margin, 0))
    shifted = jax.random.randint(jax.random.fold_in(own, 4), (count // 2,), 0, 1 << 20) % (margin + 1)
    lengths = lengths.at[donor].add(-shifted).at[sink].add(shifted)
    members = jnp.searchsorted(jnp.cumsum(lengths), jnp.arange(rows * top), side="right").astype(jnp.int32)
    grid = members.reshape(top, rows).T
    grid = grid[jax.random.permutation(jax.random.fold_in(own, 1), rows)]
    offset_by = jax.random.randint(jax.random.fold_in(own, 2), (rows, 1), 0, top)
    return jnp.take_along_axis(grid, (jnp.arange(top)[None, :] + offset_by) % top, axis=1)


def load_shares(count, total, bound, skew, full):
    portions = [(1 << 20) // math.isqrt(grade ** skew) + 1 for grade in range(1, count + 1)]
    largest = bound if full else min(bound, max(-(-total // count), total * portions[0] // sum(portions)))
    least = 1 if total - largest >= count - 1 else 0
    holding, spare = [largest] + [least] * (count - 1), total - largest - least * (count - 1)
    while spare > 0:
        free = [i for i in range(1, count) if holding[i] < largest] or [i for i in range(1, count) if holding[i] < bound]
        mass, remaining = sum([portions[i] for i in free]), spare
        for i in free:
            addition = min(bound - holding[i], max(1, remaining * portions[i] // mass), spare)
            holding[i] = holding[i] + addition
            spare = spare - addition
    return np.array(holding)


def gaussian(stream_key, extent, scale, bound, split=(), dtype=jnp.bfloat16):
    level = steps_of(stream_key, extent, split, -0.22, 0.18) if split else 1.0
    values = jax.random.normal(stream_key, extent, jnp.float32) * scale * level
    return jnp.minimum(jnp.maximum(values, -bound), bound).astype(dtype)


def setup_inputs(seed: int = 0) -> dict:
    key_of = jax.random.split(jax.random.key(seed), 8)
    block_values = gaussian(key_of[0], (N_COL, BLOCK_ROWS, BLOCK_LEN), 1.0, 6.0, ((0, 4), (1, 8)))
    block_shifts = jnp.clip(jax.random.uniform(key_of[1], (N_COL, BLOCK_ROWS, BLOCK_LEN), jnp.float32, -1.0, 1.0) * steps_of(key_of[1], (N_COL, BLOCK_ROWS, BLOCK_LEN), ((0, 4), (1, 8)), -0.4, 0.0), -1.0, 1.0).astype(jnp.bfloat16)
    block_sensor = plant(jax.random.randint(key_of[2], (N_COL, BLOCK_ROWS), 0, GROUP_SENSORS), jax.random.fold_in(key_of[2], 1), 0, GROUP_SENSORS - 1).astype(jnp.int32)
    block_window = plant(jax.random.randint(key_of[3], (N_COL, BLOCK_ROWS), 0, WINDOWS), jax.random.fold_in(key_of[3], 1), 0, WINDOWS - 1).astype(jnp.int32)
    block_owner_keys = jax.random.split(jax.random.fold_in(key_of[4], 1), N_COL * BLOCK_ROWS // BLOCKS_DEV)
    block_owner_turns = jax.random.permutation(jax.random.fold_in(key_of[4], 3), N_COL * BLOCK_ROWS // BLOCKS_DEV)
    block_owner = jax.vmap(lambda own, number: deal_out(jax.random.fold_in(key_of[4], 2), own, number, BLOCKS_DEV, N_TM, 1, CAPACITY, 2))(block_owner_keys, block_owner_turns).reshape((N_COL, BLOCK_ROWS, 1))
    block_counts = plant(jax.random.randint(key_of[5], (N_COL, N_TM), 3 * BLOCKS_DEV // 4, BLOCKS_DEV + 1), jax.random.fold_in(key_of[5], 1), 3 * BLOCKS_DEV // 4, BLOCKS_DEV).astype(jnp.int32)
    calibration = gaussian(key_of[6], (SENSORS, OUTPUTS), SENSORS ** -0.5, 0.046875, ((0, 8), (1, 4)))
    return dict(block_values=block_values, block_shifts=block_shifts, block_sensor=block_sensor, block_window=block_window, block_owner=block_owner, block_counts=block_counts, calibration=calibration)


def spread_samples(values, shifts):
    samples = values.astype(jnp.float32)
    offsets = shifts.astype(jnp.float32)
    result = jnp.zeros(samples.shape, jnp.float32)
    lead = [(0, 0)] * (samples.ndim - 1)
    for displace in (-1, 0, 1):
        weight = jnp.maximum(0.0, 1.0 - jnp.abs(offsets - displace)).astype(jnp.bfloat16)
        weight = lax.optimization_barrier(weight).astype(jnp.float32)
        product = weight * samples
        if displace == 1:
            result = result + jnp.pad(product[..., :-1], lead + [(1, 0)])
        elif displace == -1:
            result = result + jnp.pad(product[..., 1:], lead + [(0, 1)])
        else:
            result = result + product
    return result


def reference(block_values, block_shifts, block_sensor, block_window, block_owner, block_counts, calibration):
    length = block_values.shape[2]
    local_index = lax.broadcasted_iota(jnp.int32, (N_COL, BLOCK_ROWS), 1) % BLOCKS_DEV
    counts_rep = jnp.repeat(block_counts, BLOCKS_DEV, axis=1)
    is_live = (local_index < counts_rep).astype(jnp.float32)
    contribution = spread_samples(block_values, block_shifts) * is_live[:, :, None]
    col_base = lax.broadcasted_iota(jnp.int32, (N_COL, BLOCK_ROWS), 0) * GROUP_SENSORS
    row_keys = (block_owner[:, :, 0] * WINDOWS + block_window) * SENSORS + col_base + block_sensor
    summed = jnp.zeros((N_TM * WINDOWS * SENSORS, length), jnp.float32)
    summed = summed.at[row_keys.reshape(-1)].add(contribution.reshape(-1, length))
    aligned = summed.reshape(N_TM * WINDOWS, SENSORS, length).transpose(0, 2, 1)
    aligned = aligned.reshape(GRID_ROWS, SENSORS).astype(jnp.bfloat16)
    return jnp.dot(aligned, calibration, preferred_element_type=jnp.float32).astype(jnp.bfloat16)
```

```python
import functools

import jax
import jax.numpy as jnp
from jax import lax
from jax.experimental import pallas as pl
from jax.experimental.pallas import tpu as pltpu
from jax.sharding import PartitionSpec as P

WINDOWS = 4
LANES = 128
META = 32
DEPTH = 256
STEP = 32
PIECE = 256
EARLY = 1


ANY = pl.BlockSpec(memory_space=pl.ANY)
VMEM = pl.BlockSpec(memory_space=pltpu.VMEM)
MESH = pl.DeviceIdType.MESH


def spread_samples(values, shifts):
    samples = values.astype(jnp.float32)
    offsets = shifts.astype(jnp.float32)
    result = jnp.zeros(samples.shape, jnp.float32)
    lead = [(0, 0)] * (samples.ndim - 1)
    for displace in (-1, 0, 1):
        weight = jnp.maximum(0.0, 1.0 - jnp.abs(offsets - displace)).astype(jnp.bfloat16)
        weight = lax.optimization_barrier(weight).astype(jnp.float32)
        product = weight * samples
        if displace == 1:
            result = result + jnp.pad(product[..., :-1], lead + [(1, 0)])
        elif displace == -1:
            result = jnp.pad(product[..., 1:], lead + [(0, 1)])
        else:
            result = result + product
    return result


def sort_blocks(values, shifts, sensor, window, owner, count, rows, ratio, planes, capacity):
    blocks, length = values.shape
    room = planes * capacity
    bins = planes * WINDOWS * ratio
    contribution = spread_samples(values, shifts).astype(jnp.bfloat16)
    index = lax.iota(jnp.int32, blocks)
    lot = owner % ratio
    number = ((owner // ratio) * WINDOWS + window) * ratio + sensor // rows
    number = jnp.where(index < count, lot * bins + number, ratio * bins)
    key = number * blocks + index
    rank = jnp.sum((key[None, :] < key[:, None]).astype(jnp.int32), axis=1)
    edges = jnp.sum(
        (number[None, :] < lax.iota(jnp.int32, ratio * bins)[:, None]).astype(jnp.int32), axis=1
    )
    live = jnp.sum((number < ratio * bins).astype(jnp.int32))
    begin = edges[::bins]
    spot = jnp.full((blocks,), ratio * room, jnp.int32)
    for part in range(ratio):
        here = (number >= part * bins) & (number < (part + 1) * bins)
        spot = jnp.where(here, rank - begin[part] + part * room, spot)
    place = (spot[None, :] == lax.iota(jnp.int32, ratio * room)[:, None]).astype(jnp.bfloat16)
    local = sensor % rows
    payload = jnp.concatenate(
        (
            contribution,
            (local // LANES).astype(jnp.bfloat16)[:, None],
            (local % LANES).astype(jnp.bfloat16)[:, None],
            jnp.zeros((blocks, LANES - 2), jnp.bfloat16),
        ),
        axis=1,
    )
    placed = jnp.dot(place, payload, preferred_element_type=jnp.float32).reshape(ratio, room, 2 * LANES)
    ends = jnp.concatenate((edges, live[None]))
    bounds = jnp.stack([ends[p * bins:(p + 1) * bins + 1] - begin[p] for p in range(ratio)])
    bounds = jnp.pad(bounds, ((0, 0), (0, LANES - bins - 1)))[:, None, :]
    meta = jnp.concatenate(
        (
            placed[:, :, LANES].reshape(ratio, -1, LANES),
            placed[:, :, LANES + 1].reshape(ratio, -1, LANES),
            (bounds // 64).astype(jnp.float32),
            (bounds % 64).astype(jnp.float32),
        ),
        axis=1,
    )
    meta = jnp.pad(meta, ((0, 0), (0, META - meta.shape[1]), (0, 0)))
    return jnp.concatenate((placed[:, :, :LANES], meta), axis=1).astype(jnp.bfloat16)


def deliver_kernel(owners, cols, parcel, held, send_sems, recv_sems, pass_sems, own_sem):
    ratio = owners // cols
    chips = cols // 2
    t, c = lax.axis_index("tm"), lax.axis_index("col")
    core = lax.rem(c, 2)
    plane = t // ratio
    first = core == lax.rem(plane, 2)

    def out_copy(lot, chip):
        return pltpu.make_async_remote_copy(
            src_ref=parcel.at[lot],
            dst_ref=held.at[t],
            send_sem=send_sems.at[lot * chips + chip],
            recv_sem=recv_sems.at[t],
            device_id=(c * ratio + lot, chip * 2 + core),
            device_id_type=MESH,
        )

    def own_copy():
        return pltpu.make_async_copy(parcel.at[lax.rem(t, ratio)], held.at[t], own_sem)

    def pass_copy(source):
        return pltpu.make_async_remote_copy(
            src_ref=held.at[source],
            dst_ref=held.at[source],
            send_sem=pass_sems.at[source],
            recv_sem=recv_sems.at[source],
            device_id=(t, c + 1 - 2 * core),
            device_id_type=MESH,
        )

    def each_target(act):
        for lot in range(ratio):
            for chip in range(chips):
                mine = (c * ratio + lot == t) & (chip * 2 + core == c)

                @pl.when(jnp.logical_not(mine))
                def _():
                    act(out_copy(lot, chip))

    each_target(lambda copy: copy.start())
    own = plane == c

    @pl.when(own)
    def _():
        own_copy().start()

    for step in range(owners):
        source = lax.rem(t + step, owners)
        if step == 0:

            @pl.when(first & own)
            def _():
                own_copy().wait()

            @pl.when(first & jnp.logical_not(own))
            def _():
                pass_copy(source).wait_recv()

        else:

            @pl.when(first)
            def _():
                pass_copy(source).wait_recv()

        @pl.when(first)
        def _():
            pass_copy(source).start()

    each_target(lambda copy: copy.wait_send())
    for source in range(owners):

        @pl.when(first)
        def _():
            pass_copy(source).wait_send()

        @pl.when(jnp.logical_not(first))
        def _():
            pass_copy(source).wait_recv()


def deliver(parcel, owners, cols):
    ratio = owners // cols
    return pl.pallas_call(
        functools.partial(deliver_kernel, owners, cols),
        out_shape=jax.ShapeDtypeStruct((owners,) + parcel.shape[1:], parcel.dtype),
        in_specs=[VMEM],
        out_specs=ANY,
        scratch_shapes=[
            pltpu.SemaphoreType.DMA((ratio * (cols // 2),)),
            pltpu.SemaphoreType.DMA((owners,)),
            pltpu.SemaphoreType.DMA((owners,)),
            pltpu.SemaphoreType.DMA,
        ],
        compiler_params=pltpu.CompilerParams(has_side_effects=True, vmem_limit_bytes=16 * 1024 * 1024),
        cost_estimate=pl.CostEstimate(flops=10 * 10**9, bytes_accessed=10**7, transcendentals=0),
        name="deliver",
    )(parcel)


def align_kernel(cfg, held, aligned, raw, limit, limit_s, contrib, names, stage, tags, total, ready, sems, out_sems):
    sources, room, rows, ratio, planes, deep = cfg
    bins = planes * WINDOWS * ratio
    lot = lax.rem(lax.axis_index("tm"), ratio)
    height = room + META
    third = room // LANES
    loads = [
        pltpu.make_async_copy(held.at[s], raw.at[pl.ds(s * height, height)], sems.at[s])
        for s in range(sources)
    ]
    for load in loads:
        load.start()
    stage[...] = jnp.zeros_like(stage)
    tags[...] = jnp.zeros_like(tags)
    tail = pl.ds(sources * room, contrib.shape[0] - sources * room)
    contrib[tail, :] = jnp.zeros_like(contrib[tail, :])
    names[tail, :] = jnp.zeros_like(names[tail, :])
    for s in range(sources):
        loads[s].wait()
        meta = raw[pl.ds(s * height + room, META), :].astype(jnp.float32)
        limit[pl.ds(s, 1), :] = (
            meta[2 * third:2 * third + 1] * 64.0 + meta[2 * third + 1:2 * third + 2]
        ).astype(jnp.int32)
        for r in range(third):
            tag = meta[r:r + 1] * float(LANES) + meta[third + r:third + r + 1]
            at = pl.ds(s * room + r * LANES, LANES)
            names[at, :] = jnp.transpose(jnp.broadcast_to(tag, (LANES, LANES)))
            contrib[at, :] = raw[pl.ds(s * height + r * LANES, LANES), :].astype(jnp.float32)
    fetch = pltpu.make_async_copy(limit, limit_s, sems.at[sources])
    fetch.start()
    fetch.wait()
    lane = lax.broadcasted_iota(jnp.int32, (1, LANES), 1)
    row = lax.broadcasted_iota(jnp.int32, (DEPTH, LANES), 0)

    def put(number, slot):
        window, half = number // ratio, lax.rem(number, ratio)
        return pltpu.make_async_copy(
            ready.at[slot],
            aligned.at[
                window // WINDOWS,
                lax.rem(half - lot + ratio, ratio),
                pl.ds(pl.multiple_of(lax.rem(window, WINDOWS) * LANES, LANES), LANES),
            ],
            out_sems.at[slot],
        )

    def one_bin(number, carry):
        slot = lax.rem(number, 2)

        @pl.when(number >= 2)
        def _():
            put(number - 2, slot).wait()

        count = jnp.int32(0)
        for s in range(sources):
            begin = limit_s[s, number]
            extent = limit_s[s, number + 1] - begin

            def copy_rows(step, inner, s=s, begin=begin, count=count):
                source = pl.ds(s * room + begin + step * STEP, STEP)
                target = pl.ds(count + step * STEP, STEP)
                stage[target, :] = contrib[source, :]
                tags[target, :] = names[source, :]
                return inner

            lax.fori_loop(0, (extent + STEP - 1) // STEP, copy_rows, 0)
            count = count + extent

        def chunk(at, write):
            place = pl.ds(pl.multiple_of(at * DEPTH, DEPTH), DEPTH)
            left = jnp.transpose(stage[place, :]).astype(jnp.bfloat16)
            tag = jnp.where(row + at * DEPTH < count, tags[place, :], -1.0).astype(jnp.int32)
            wide = 4 * LANES
            for n in range(rows // wide):
                hot = jnp.concatenate(
                    [
                        (tag == lane + (n * wide + k * LANES)).astype(jnp.float32).astype(jnp.bfloat16)
                        for k in range(wide // LANES)
                    ],
                    axis=1,
                )
                write(
                    pl.ds(n * wide, wide),
                    jnp.dot(left, hot, preferred_element_type=jnp.float32),
                )

        @pl.when(count <= DEPTH)
        def _():
            def write(span, value):
                ready[slot, :, span] = value.astype(jnp.bfloat16)

            chunk(0, write)

        @pl.when(count > DEPTH)
        def _():
            total[...] = jnp.zeros_like(total)

            def write(span, value):
                total[:, span] += value

            def more(at, inner):
                chunk(at, write)
                return inner

            lax.fori_loop(0, (count + DEPTH - 1) // DEPTH, more, 0)
            ready[slot] = total[...].astype(jnp.bfloat16)

        put(number, slot).start()
        return carry

    lax.fori_loop(0, bins, one_bin, 0)
    for number in (bins - 2, bins - 1):
        put(number, number % 2).wait()


def align(held, rows, ratio, planes, capacity):
    sources, height, length = held.shape
    room = height - META
    deep = -(-(sources * capacity + STEP) // DEPTH) * DEPTH
    cfg = (sources, room, rows, ratio, planes, deep)
    return pl.pallas_call(
        functools.partial(align_kernel, cfg),
        out_shape=jax.ShapeDtypeStruct((planes, ratio, WINDOWS * length, rows), jnp.bfloat16),
        in_specs=[ANY],
        out_specs=ANY,
        scratch_shapes=[
            pltpu.VMEM((sources * height, length), jnp.bfloat16),
            pltpu.VMEM((sources, LANES), jnp.int32),
            pltpu.SMEM((sources, LANES), jnp.int32),
            pltpu.VMEM((sources * room + STEP, length), jnp.float32),
            pltpu.VMEM((sources * room + STEP, LANES), jnp.float32),
            pltpu.VMEM((deep, length), jnp.float32),
            pltpu.VMEM((deep, LANES), jnp.float32),
            pltpu.VMEM((length, rows), jnp.float32),
            pltpu.VMEM((2, length, rows), jnp.bfloat16),
            pltpu.SemaphoreType.DMA((sources + 1,)),
            pltpu.SemaphoreType.DMA((2,)),
        ],
        compiler_params=pltpu.CompilerParams(vmem_limit_bytes=58 * 1024 * 1024),
        cost_estimate=pl.CostEstimate(flops=10 * 10**9, bytes_accessed=2 * 10**7, transcendentals=0),
        name="align",
    )(held)


def far_first(planes):
    return [sorted(range(planes), key=lambda p: (-abs(p - z), -p)) for z in range(planes)]


def reduce_kernel(
    cfg, aligned, calib, early, out, left, near, far, stage, up, down, kept, total, answer,
    local_sems, far_send, far_recv, up_send, up_recv, down_send, down_recv, out_sems,
):
    planes, ratio, pieces, prior = cfg
    t, c = lax.axis_index("tm"), lax.axis_index("col")
    plane, lot = t // ratio, lax.rem(t, ratio)
    height = left.shape[2]

    def far_copy(step, piece):
        return pltpu.make_async_remote_copy(
            src_ref=calib.at[:, pl.ds(pl.multiple_of(piece * PIECE, PIECE), PIECE)],
            dst_ref=far.at[step - 1, piece],
            send_sem=far_send.at[step - 1, piece],
            recv_sem=far_recv.at[step - 1, piece],
            device_id=(plane * ratio + lax.rem(lot - step + ratio, ratio), c),
            device_id_type=MESH,
        )

    for piece in range(prior, pieces):
        for step in range(1, ratio):
            far_copy(step, piece).start()

    order = far_first(planes)

    def target(turn):
        chosen = jnp.int32(0)
        for z in range(planes):
            row = jnp.int32(0)
            for k in range(planes):
                row = row + jnp.where(turn == k, order[z][k], 0)
            chosen = chosen + jnp.where(plane == z, row, 0)
        return chosen

    near_load = [
        pltpu.make_async_copy(
            calib.at[:, pl.ds(piece * PIECE, PIECE)], near.at[piece], local_sems.at[piece]
        )
        for piece in range(pieces)
    ]
    early_load = [
        pltpu.make_async_copy(
            early.at[step - 1, :, pl.ds(piece * PIECE, PIECE)],
            far.at[step - 1, piece],
            local_sems.at[pieces + planes + (step - 1) * prior + piece],
        )
        for piece in range(prior)
        for step in range(1, ratio)
    ]

    def left_load(turn):
        where = target(turn)
        return pltpu.make_async_copy(
            aligned.at[where], left.at[where], local_sems.at[pieces + turn]
        )

    left_load(0).start()
    near_load[0].start()
    for load in early_load:
        load.start()
    for turn in range(1, planes):
        left_load(turn).start()
    for load in near_load[1:]:
        load.start()
    near_load[0].wait()
    for load in early_load:
        load.wait()

    def hop(piece, where, buffer, sends, recvs, side):
        return pltpu.make_async_remote_copy(
            src_ref=stage.at[piece, where],
            dst_ref=buffer.at[piece, where],
            send_sem=sends.at[piece, where],
            recv_sem=recvs.at[piece, where],
            device_id=(t + side * ratio, c),
            device_id_type=MESH,
        )

    def go_up(piece, where):
        return hop(piece, where, up, up_send, up_recv, 1)

    def go_down(piece, where):
        return hop(piece, where, down, down_send, down_recv, -1)

    def one_piece(piece, carry):
        @pl.when(piece > 0)
        def _():
            pltpu.make_async_copy(
                calib.at[:, pl.ds(pl.multiple_of(piece * PIECE, PIECE), PIECE)],
                near.at[piece],
                local_sems.at[piece],
            ).wait()

        @pl.when(piece >= prior)
        def _():
            for step in range(1, ratio):
                far_copy(step, piece).wait_recv()

        def one_turn(turn, inner):
            where = target(turn)

            @pl.when(piece == 0)
            def _():
                pltpu.make_async_copy(
                    aligned.at[where], left.at[where], local_sems.at[pieces + turn]
                ).wait()

            value = jnp.dot(left[where, 0], near[piece], preferred_element_type=jnp.float32)
            for step in range(1, ratio):
                value = value + jnp.dot(
                    left[where, step], far[step - 1, piece], preferred_element_type=jnp.float32
                )
            total[...] = value

            @pl.when((where > plane) & (plane > 0))
            def _():
                go_up(piece, where).wait_recv()
                stage[piece, where] = (total[...] + up[piece, where].astype(jnp.float32)).astype(jnp.bfloat16)

            @pl.when((where < plane) & (plane < planes - 1))
            def _():
                go_down(piece, where).wait_recv()
                stage[piece, where] = (total[...] + down[piece, where].astype(jnp.float32)).astype(jnp.bfloat16)

            @pl.when(((where > plane) & (plane == 0)) | ((where < plane) & (plane == planes - 1)))
            def _():
                stage[piece, where] = total[...].astype(jnp.bfloat16)

            @pl.when(where > plane)
            def _():
                go_up(piece, where).start()

            @pl.when(where < plane)
            def _():
                go_down(piece, where).start()

            @pl.when(where == plane)
            def _():
                kept[piece] = total[...]

            return inner

        lax.fori_loop(0, planes, one_turn, 0)
        return carry

    lax.fori_loop(0, pieces, one_piece, 0)

    def put(piece):
        return pltpu.make_async_copy(
            answer.at[piece],
            out.at[:, pl.ds(pl.multiple_of(piece * PIECE, PIECE), PIECE)],
            out_sems.at[piece],
        )

    def finish(piece, carry):
        @pl.when(plane > 0)
        def _():
            go_up(piece, plane).wait_recv()
            kept[piece] += up[piece, plane].astype(jnp.float32)

        @pl.when(plane < planes - 1)
        def _():
            go_down(piece, plane).wait_recv()
            kept[piece] += down[piece, plane].astype(jnp.float32)

        answer[piece] = kept[piece].astype(jnp.bfloat16)
        put(piece).start()
        return carry

    lax.fori_loop(0, pieces, finish, 0)

    def drain(piece, carry):
        put(piece).wait()
        for where in range(planes):
            @pl.when(where > plane)
            def _():
                go_up(piece, where).wait_send()

            @pl.when(where < plane)
            def _():
                go_down(piece, where).wait_send()

        @pl.when(piece >= prior)
        def _():
            for step in range(1, ratio):
                far_copy(step, piece).wait_send()

        return carry

    lax.fori_loop(0, pieces, drain, 0)


def reduce(aligned, calib, early):
    planes, ratio, height, rows = aligned.shape
    outputs = calib.shape[1]
    pieces = outputs // PIECE
    prior = early.shape[2] // PIECE
    cfg = (planes, ratio, pieces, prior)
    hops = (pieces, planes)
    return pl.pallas_call(
        functools.partial(reduce_kernel, cfg),
        out_shape=jax.ShapeDtypeStruct((height, outputs), jnp.bfloat16),
        in_specs=[ANY, ANY, ANY],
        out_specs=ANY,
        scratch_shapes=[
            pltpu.VMEM((planes, ratio, height, rows), jnp.bfloat16),
            pltpu.VMEM((pieces, rows, PIECE), jnp.bfloat16),
            pltpu.VMEM((ratio - 1, pieces, rows, PIECE), jnp.bfloat16),
            pltpu.VMEM((pieces, planes, height, PIECE), jnp.bfloat16),
            pltpu.VMEM((pieces, planes, height, PIECE), jnp.bfloat16),
            pltpu.VMEM((pieces, planes, height, PIECE), jnp.bfloat16),
            pltpu.VMEM((pieces, height, PIECE), jnp.float32),
            pltpu.VMEM((height, PIECE), jnp.float32),
            pltpu.VMEM((pieces, height, PIECE), jnp.bfloat16),
            pltpu.SemaphoreType.DMA((pieces + planes + ratio * prior,)),
            pltpu.SemaphoreType.DMA((ratio - 1, pieces)),
            pltpu.SemaphoreType.DMA((ratio - 1, pieces)),
            pltpu.SemaphoreType.DMA(hops),
            pltpu.SemaphoreType.DMA(hops),
            pltpu.SemaphoreType.DMA(hops),
            pltpu.SemaphoreType.DMA(hops),
            pltpu.SemaphoreType.DMA((pieces,)),
        ],
        compiler_params=pltpu.CompilerParams(has_side_effects=True, vmem_limit_bytes=60 * 1024 * 1024),
        cost_estimate=pl.CostEstimate(flops=20 * 10**9, bytes_accessed=3 * 10**7, transcendentals=0),
        name="reduce",
    )(aligned, calib, early)


def per_device(
    block_values, block_shifts, block_sensor, block_window, block_owner, block_counts, calibration
):
    owners = lax.axis_size("tm")
    cols = lax.axis_size("col")
    ratio = owners // cols
    planes = owners // ratio
    rows, outputs = calibration.shape
    blocks = block_values.shape[1]
    capacity = min(blocks, blocks * 3 // (2 * owners))
    prior = EARLY * PIECE

    def shifted(step):
        return [((t // ratio) * ratio + (t % ratio + step) % ratio, t) for t in range(owners)]

    early = jnp.stack(
        [lax.ppermute(calibration[:, :prior], "tm", shifted(step)) for step in range(1, ratio)]
    )
    parcel = sort_blocks(
        block_values[0], block_shifts[0], block_sensor[0], block_window[0], block_owner[0, :, 0],
        block_counts[0, 0], rows, ratio, planes, capacity,
    )
    held = deliver(parcel, owners, cols)
    aligned = align(held, rows, ratio, planes, capacity)
    return reduce(aligned, calibration, early)


def solution(mesh):
    placed = (
        P("col", "tm", None),
        P("col", "tm", None),
        P("col", "tm"),
        P("col", "tm"),
        P("col", "tm", None),
        P("col", "tm"),
        P("tm", "col"),
    )
    return jax.shard_map(
        per_device, mesh=mesh, in_specs=placed, out_specs=P("tm", "col"), check_vma=False
    )
```

```python
import functools

import jax
import jax.numpy as jnp
from jax import lax
from jax.experimental import pallas as pl
from jax.experimental.pallas import tpu as pltpu
from jax.sharding import PartitionSpec as P

WINDOWS = 4
LANES = 128
META = 32
DEPTH = 256
STEP = 48
PIECE = 256
GRANT = 67_000_000


ANY = pl.BlockSpec(memory_space=pl.ANY)
VMEM = pl.BlockSpec(memory_space=pltpu.VMEM)
MESH = pl.DeviceIdType.MESH


def cut(whole, size):
    return jnp.floor((whole + 0.5) * (1.0 / size))


def near_first(groups):
    return [sorted(range(groups), key=lambda g: (abs(g - me), g)) for me in range(groups)]


def pick(table, mine, turn):
    chosen = jnp.int32(0)
    for own, row in enumerate(table):
        value = jnp.int32(0)
        for at, entry in enumerate(row):
            value = value + jnp.where(turn == at, entry, 0)
        chosen = chosen + jnp.where(mine == own, value, 0)
    return chosen


def spread_rows(values, shifts):
    samples = values.astype(jnp.float32)
    offsets = shifts.astype(jnp.float32)
    lane = lax.broadcasted_iota(jnp.int32, samples.shape, 1)
    result = None
    for displace in (-1, 0, 1):
        weight = jnp.maximum(0.0, 1.0 - jnp.abs(offsets - displace)).astype(jnp.bfloat16)
        product = weight.astype(jnp.float32) * samples
        if displace == 1:
            product = jnp.where(lane == 0, 0.0, pltpu.roll(product, 1, 1))
        elif displace == -1:
            product = jnp.where(lane == LANES - 1, 0.0, pltpu.roll(product, LANES - 1, 1))
        result = product if result is None else result + product
    return result


def sort_blocks(cfg, values, shifts, sensor, window, owner, count, parcel, payload, bases, tops, notes, send):
    owners, cols, rows, room = cfg
    ratio = owners // cols
    planes = owners // ratio
    groups = sensor.shape[0]
    bins = planes * WINDOWS * ratio
    every = ratio * bins
    third = room // LANES
    lane = lax.broadcasted_iota(jnp.int32, (1, LANES), 1).astype(jnp.float32)
    down = lax.broadcasted_iota(jnp.int32, (LANES, LANES), 0).astype(jnp.float32)
    index = (
        lax.broadcasted_iota(jnp.int32, (groups, LANES), 0) * LANES
        + lax.broadcasted_iota(jnp.int32, (groups, LANES), 1)
    )
    live = index < count[...]
    who = owner[...].astype(jnp.float32)
    what = sensor[...].astype(jnp.float32)
    where = cut(who, ratio)
    half = cut(what, rows)
    number = (where * WINDOWS + window[...].astype(jnp.float32)) * ratio + half
    number = jnp.where(live, (who - ratio * where) * bins + number, -1.0)
    local = what - rows * half
    local_top = cut(local, LANES)
    local_low = local - LANES * local_top
    bin_row = lax.broadcasted_iota(jnp.int32, (every, LANES), 0).astype(jnp.float32)
    hot = [jnp.where(number[r:r + 1] == bin_row, 1.0, 0.0) for r in range(groups)]
    before = jnp.concatenate([jnp.where(down < lane, 1.0, 0.0), jnp.ones((LANES, LANES), jnp.float32)], axis=1)
    earlier = jnp.dot(
        jnp.concatenate(hot, axis=0).astype(jnp.bfloat16), before.astype(jnp.bfloat16),
        preferred_element_type=jnp.float32,
    )
    run = jnp.zeros((every, LANES), jnp.float32)
    offset = []
    for r in range(groups):
        part = earlier[r * every:(r + 1) * every]
        offset.append(run + part[:, :LANES])
        run = run + part[:, LANES:]
    upto = run
    shift = 1
    while shift < every:
        upto = upto + jnp.where(bin_row >= shift, pltpu.roll(upto, shift, 0), 0.0)
        shift *= 2
    begin = upto - run
    begin = jnp.concatenate(
        [begin[p * bins:(p + 1) * bins] - begin[p * bins:p * bins + 1] for p in range(ratio)], axis=0
    )
    end = begin + run
    lot_of = cut(bin_row, bins)
    first = begin + lot_of * room
    for r in range(groups):
        spot = jnp.sum(hot[r] * (first + offset[r]), axis=0, keepdims=True)
        spot = jnp.where(live[r:r + 1], spot, -1.0)
        top = cut(jnp.maximum(spot, 0.0), LANES)
        tops[r:r + 1, :] = jnp.where(spot < 0.0, -1.0, top)
        bases[:, r * LANES:(r + 1) * LANES] = jnp.where(spot - top * LANES == down, 1.0, 0.0).astype(jnp.bfloat16)
        at = pl.ds(r * LANES, LANES)
        payload[at, :LANES] = spread_rows(values[at, :], shifts[at, :]).astype(jnp.bfloat16)
        tag = jnp.where(
            down < LANES // 2,
            jnp.broadcast_to(local_top[r:r + 1], (LANES, LANES)),
            jnp.broadcast_to(local_low[r:r + 1], (LANES, LANES)),
        )
        payload[at, LANES:] = jnp.transpose(tag).astype(jnp.bfloat16)
    edge = []
    for column in (begin, end):
        if every < LANES:
            column = jnp.concatenate([column, jnp.zeros((LANES - every, LANES), jnp.float32)], axis=0)
        row = jnp.transpose(column)[0:1]
        high = cut(row, 64)
        edge += [high, row - 64 * high]
    notes[...] = jnp.zeros_like(notes)
    for p in range(ratio):
        for k, row in enumerate(edge):
            notes[p, 2 * third + k:2 * third + k + 1, :] = row
    tile = 4 * LANES
    for p in range(ratio):

        def one_tile(step, carry, p=p):
            strips = []
            for k in range(tile // LANES):
                wanted = (step * (tile // LANES) + k + p * third).astype(jnp.float32)
                chosen = jnp.where(tops[...] == wanted, 1.0, 0.0).astype(jnp.bfloat16)
                strips.append(
                    jnp.concatenate(
                        [bases[:, r * LANES:(r + 1) * LANES] * chosen[r:r + 1] for r in range(groups)], axis=1
                    )
                )
            placed = jnp.dot(jnp.concatenate(strips, axis=0), payload[...], preferred_element_type=jnp.float32)
            parcel[p, pl.ds(pl.multiple_of(step * tile, tile), tile), :] = placed[:, :LANES].astype(jnp.bfloat16)
            for k in range(tile // LANES):
                flat = jnp.transpose(placed[k * LANES:(k + 1) * LANES, LANES:])
                at = step * (tile // LANES) + k
                notes[p, pl.ds(at, 1), :] = flat[0:1]
                notes[p, pl.ds(third + at, 1), :] = flat[LANES // 2:LANES // 2 + 1]
            return carry

        lax.fori_loop(0, room // tile, one_tile, 0)
        parcel[p, room:room + META, :] = notes[p].astype(jnp.bfloat16)
        send(p)


def greet(peers):
    barrier = pltpu.get_barrier_semaphore()
    for peer in peers:
        pl.semaphore_signal(barrier, inc=1, device_id=peer, device_id_type=MESH)
    pl.semaphore_wait(barrier, len(peers))


def deliver_kernel(
    cfg, values_in, shifts_in, sensor_in, window_in, owner_in, count, calib, held, early,
    values, shifts, sensor, window, owner, load_sems, parcel, relay, payload, bases, tops, notes, send_sems, recv_sems, relay_send, relay_recv, turn_sems,
    side_sems, pass_sems, own_sem, far_send, far_recv,
):
    owners, cols, rows, room = cfg
    ratio = owners // cols
    planes = owners // ratio
    chips = cols // 2
    t, c = lax.axis_index("tm"), lax.axis_index("col")
    core, chip = lax.rem(c, 2), c // 2
    plane, lot = t // ratio, lax.rem(t, ratio)
    first = core == lax.rem(plane, 2)

    def line_of(source, column):
        return lax.rem(source // ratio + lax.rem(source, ratio) + column, chips)

    line = line_of(t, c)
    direct = line == chip

    def far_copy(step):
        return pltpu.make_async_remote_copy(
            src_ref=calib.at[pl.ds(0, early.shape[1]), pl.ds(0, PIECE)],
            dst_ref=early.at[step - 1],
            send_sem=far_send.at[step - 1],
            recv_sem=far_recv.at[step - 1],
            device_id=(plane * ratio + lax.rem(lot - step + ratio, ratio), c),
            device_id_type=MESH,
        )

    def out_copy(target):
        return pltpu.make_async_remote_copy(
            src_ref=parcel.at[target],
            dst_ref=held.at[t],
            send_sem=send_sems.at[target],
            recv_sem=recv_sems.at[t],
            device_id=(c * ratio + target, c),
            device_id_type=MESH,
        )

    def relay_copy(target):
        return pltpu.make_async_remote_copy(
            src_ref=parcel.at[target],
            dst_ref=relay.at[chip, target],
            send_sem=relay_send.at[target],
            recv_sem=relay_recv.at[chip, target],
            device_id=(t, line * 2 + core),
            device_id_type=MESH,
        )

    def relay_arrival(origin, target):
        return pltpu.make_async_remote_copy(
            src_ref=parcel.at[target],
            dst_ref=relay.at[origin, target],
            send_sem=relay_send.at[target],
            recv_sem=relay_recv.at[origin, target],
            device_id=(t, origin * 2 + core),
            device_id_type=MESH,
        )

    def turn_copy(origin, target):
        return pltpu.make_async_remote_copy(
            src_ref=relay.at[origin, target],
            dst_ref=held.at[t],
            send_sem=turn_sems.at[origin, target],
            recv_sem=recv_sems.at[t],
            device_id=((origin * 2 + core) * ratio + target, c),
            device_id_type=MESH,
        )

    def pass_copy(source):
        return pltpu.make_async_remote_copy(
            src_ref=held.at[source],
            dst_ref=held.at[source],
            send_sem=pass_sems.at[source],
            recv_sem=recv_sems.at[source],
            device_id=(t, c + 1 - 2 * core),
            device_id_type=MESH,
        )

    def side_copy(source, step):
        return pltpu.make_async_remote_copy(
            src_ref=held.at[source],
            dst_ref=held.at[source],
            send_sem=side_sems.at[step - 1, source],
            recv_sem=recv_sems.at[source],
            device_id=(t, lax.rem(chip + step, chips) * 2 + core),
            device_id_type=MESH,
        )

    loads = [
        pltpu.make_async_copy(source, target, load_sems.at[k])
        for k, (source, target) in enumerate(
            ((owner_in, owner), (sensor_in, sensor), (window_in, window), (values_in, values), (shifts_in, shifts))
        )
    ]
    for load in loads:
        load.start()
    greet(
        [(lax.rem(t + step, owners), c) for step in range(1, owners)]
        + [(t, lax.rem(c + step, cols)) for step in range(1, cols)]
    )
    for step in range(1, ratio):
        far_copy(step).start()
    for load in loads:
        load.wait()

    def send(target):
        here = c * ratio + target == t

        @pl.when(jnp.logical_not(direct))
        def _():
            relay_copy(target).start()

        @pl.when(direct & here)
        def _():
            pltpu.make_async_copy(parcel.at[target], held.at[t], own_sem).start()

        @pl.when(direct & jnp.logical_not(here))
        def _():
            out_copy(target).start()

    sort_blocks(
        cfg, values, shifts, sensor, window, owner, count, parcel, payload, bases, tops, notes, send
    )

    def each_turn(act):
        for step in range(1, chips):
            origin = lax.rem(chip + step, chips)
            column = origin * 2 + core
            for target in range(ratio):
                here = column * ratio + target == t

                @pl.when(line_of(t, column) == chip)
                def _():
                    act(origin, target, here)

    def forward(origin, target, here):
        relay_arrival(origin, target).wait_recv()

        @pl.when(here)
        def _():
            pltpu.make_async_copy(relay.at[origin, target], held.at[t], own_sem).start()

        @pl.when(jnp.logical_not(here))
        def _():
            turn_copy(origin, target).start()

    each_turn(forward)
    table = near_first(planes)
    nearest = [
        pick(table, plane, turn) * ratio + lax.rem(lot + step, ratio)
        for turn in range(planes)
        for step in range(ratio)
    ]

    for source in nearest:
        entry = first & (line_of(source, plane) == chip)

        @pl.when(entry & (source == t))
        def _():
            pltpu.make_async_copy(parcel.at[lot], held.at[t], own_sem).wait()

        @pl.when(entry & (source != t))
        def _():
            pass_copy(source).wait_recv()

        @pl.when(entry)
        def _():
            for step in range(1, chips):
                side_copy(source, step).start()
            pass_copy(source).start()

    for source in nearest:

        @pl.when(first & (line_of(source, plane) != chip))
        def _():
            pass_copy(source).wait_recv()
            pass_copy(source).start()

    for target in range(ratio):

        @pl.when(direct & (c * ratio + target != t))
        def _():
            out_copy(target).wait_send()

        @pl.when(jnp.logical_not(direct))
        def _():
            relay_copy(target).wait_send()

    def settle(origin, target, here):
        @pl.when(jnp.logical_not(here))
        def _():
            turn_copy(origin, target).wait_send()

    each_turn(settle)

    for source in range(owners):

        @pl.when(first & (line_of(source, plane) == chip))
        def _():
            for step in range(1, chips):
                side_copy(source, step).wait_send()

        @pl.when(first)
        def _():
            pass_copy(source).wait_send()

        @pl.when(jnp.logical_not(first))
        def _():
            pass_copy(source).wait_recv()

    for step in range(1, ratio):
        far_copy(step).wait()


def deliver(values, shifts, sensor, window, owner, count, calib, owners, cols, capacity):
    ratio = owners // cols
    blocks, length = values.shape
    rows = calib.shape[0]
    room = owners // ratio * capacity
    every = owners * WINDOWS * ratio
    chips = cols // 2
    cfg = (owners, cols, rows, room)
    groups = blocks // LANES
    return pl.pallas_call(
        functools.partial(deliver_kernel, cfg),
        out_shape=[
            jax.ShapeDtypeStruct((owners, room + META, length), jnp.bfloat16),
            jax.ShapeDtypeStruct((ratio - 1, rows // 2, PIECE), jnp.bfloat16),
        ],
        in_specs=[ANY] * 5 + [VMEM, ANY],
        out_specs=[ANY, ANY],
        scratch_shapes=[
            pltpu.VMEM((blocks, length), jnp.bfloat16),
            pltpu.VMEM((blocks, length), jnp.bfloat16),
            pltpu.VMEM((groups, LANES), jnp.int32),
            pltpu.VMEM((groups, LANES), jnp.int32),
            pltpu.VMEM((groups, LANES), jnp.int32),
            pltpu.SemaphoreType.DMA((5,)),
            pltpu.VMEM((ratio, room + META, length), jnp.bfloat16),
            pltpu.VMEM((chips, ratio, room + META, length), jnp.bfloat16),
            pltpu.VMEM((blocks, 2 * LANES), jnp.bfloat16),
            pltpu.VMEM((LANES, blocks), jnp.bfloat16),
            pltpu.VMEM((groups, LANES), jnp.float32),
            pltpu.VMEM((ratio, META, LANES), jnp.float32),
            pltpu.SemaphoreType.DMA((ratio,)),
            pltpu.SemaphoreType.DMA((owners,)),
            pltpu.SemaphoreType.DMA((ratio,)),
            pltpu.SemaphoreType.DMA((chips, ratio)),
            pltpu.SemaphoreType.DMA((chips, ratio)),
            pltpu.SemaphoreType.DMA((max(chips - 1, 1), owners)),
            pltpu.SemaphoreType.DMA((owners,)),
            pltpu.SemaphoreType.DMA,
            pltpu.SemaphoreType.DMA((ratio - 1,)),
            pltpu.SemaphoreType.DMA((ratio - 1,)),
        ],
        compiler_params=pltpu.CompilerParams(
            collective_id=0, has_side_effects=True, vmem_limit_bytes=GRANT
        ),
        cost_estimate=pl.CostEstimate(flops=10 * 10**9, bytes_accessed=10**7, transcendentals=0),
        name="deliver",
    )(values, shifts, sensor, window, owner, count, calib)


def align_kernel(cfg, held, aligned, raw, limit, limit_s, contrib, names, stage, tags, total, ready, sems, out_sems):
    sources, room, rows, ratio, planes, deep = cfg
    bins = planes * WINDOWS * ratio
    lot = lax.rem(lax.axis_index("tm"), ratio)
    height = room + META
    third = room // LANES
    loads = [
        pltpu.make_async_copy(held.at[s], raw.at[pl.ds(s * height, height)], sems.at[s])
        for s in range(sources)
    ]
    for load in loads:
        load.start()
    stage[...] = jnp.zeros_like(stage)
    tags[...] = jnp.zeros_like(tags)
    tail = pl.ds(sources * room, contrib.shape[0] - sources * room)
    contrib[tail, :] = jnp.zeros_like(contrib[tail, :])
    names[tail, :] = jnp.zeros_like(names[tail, :])
    for s in range(sources):
        loads[s].wait()
        meta = raw[pl.ds(s * height + room, META), :].astype(jnp.float32)
        for side in range(2):
            at = 2 * third + 2 * side
            limit[pl.ds(side * sources + s, 1), :] = (
                meta[at:at + 1] * 64.0 + meta[at + 1:at + 2]
            ).astype(jnp.int32)
        for r in range(third):
            tag = meta[r:r + 1] * float(LANES) + meta[third + r:third + r + 1]
            at = pl.ds(s * room + r * LANES, LANES)
            names[at, :] = jnp.transpose(jnp.broadcast_to(tag, (LANES, LANES)))
            contrib[at, :] = raw[pl.ds(s * height + r * LANES, LANES), :].astype(jnp.float32)
    fetch = pltpu.make_async_copy(limit, limit_s, sems.at[sources])
    fetch.start()
    fetch.wait()
    def put(window, half):
        turn = lax.rem(window, 2)
        return pltpu.make_async_copy(
            ready.at[turn, half],
            aligned.at[
                window // WINDOWS,
                lax.rem(half - lot + ratio, ratio),
                pl.ds(pl.multiple_of(lax.rem(window, WINDOWS) * LANES, LANES), LANES),
            ],
            out_sems.at[turn, half],
        )

    def copy_rows(source, target, half, extent):
        stage[half, pl.ds(target, extent), :] = contrib[pl.ds(source, extent), :]
        tags[half, pl.ds(target, extent), :] = names[pl.ds(source, extent), :]

    def spans_of(window, half):
        number = lot * bins + window * ratio + half
        count, longest = 0, 0
        spans = []
        for s in range(sources):
            begin = limit_s[s, number]
            extent = limit_s[sources + s, number] - begin
            spans.append((s * room + begin, count, extent))
            count = count + extent
            longest = jnp.maximum(longest, extent)
        return count, longest, spans

    def merge(half, longest, spans):
        def straight(size):
            for source, target, _ in spans:
                copy_rows(source, target, half, size)

        for low, high in ((-1, STEP // 2), (STEP // 2, STEP), (STEP, 2 * STEP)):

            @pl.when((longest > low) & (longest <= high))
            def _():
                straight(high)

        @pl.when(longest > 2 * STEP)
        def _():
            for source, target, extent in spans:

                def more(step, inner, source=source, target=target):
                    copy_rows(source + step * STEP, target + step * STEP, half, STEP)
                    return inner

                lax.fori_loop(0, (extent + STEP - 1) // STEP, more, 0)

    def chunk(half, at, size, count, write):
        place = pl.ds(pl.multiple_of(at * size, size), size)
        left = jnp.transpose(stage[half, place, :]).astype(jnp.bfloat16)
        tag = tags[half, place, :]
        top = jnp.floor(tag * (1.0 / LANES))
        low = tag - top * LANES
        lane = lax.broadcasted_iota(jnp.int32, (size, LANES), 1).astype(jnp.float32)
        row = lax.broadcasted_iota(jnp.int32, (size, LANES), 0)
        base = jnp.where((low == lane) & (row + at * size < count), 1.0, 0.0).astype(jnp.bfloat16)
        top = top.astype(jnp.bfloat16)
        nothing = jnp.zeros_like(base)
        wide = 4 * LANES
        for n in range(rows // wide):
            hot = jnp.concatenate(
                [
                    jnp.where(top == jnp.bfloat16(n * (wide // LANES) + k), base, nothing)
                    for k in range(wide // LANES)
                ],
                axis=1,
            )
            write(pl.ds(n * wide, wide), jnp.dot(left, hot, preferred_element_type=jnp.float32))

    def one_window(window, carry):
        turn = lax.rem(window, 2)

        @pl.when(window >= 2)
        def _():
            for half in range(ratio):
                put(window - 2, half).wait()

        for half in range(ratio):
            count, longest, spans = spans_of(window, half)
            merge(half, longest, spans)

            def store(span, value, half=half):
                ready[turn, half, :, span] = value.astype(jnp.bfloat16)

            @pl.when(count <= DEPTH)
            def _():
                chunk(half, 0, DEPTH, count, store)

            @pl.when((count > DEPTH) & (count <= 2 * DEPTH))
            def _():
                chunk(half, 0, 2 * DEPTH, count, store)

            @pl.when(count > 2 * DEPTH)
            def _():
                total[...] = jnp.zeros_like(total)

                def add(span, value):
                    total[:, span] += value

                def more(at, inner):
                    chunk(half, at, DEPTH, count, add)
                    return inner

                lax.fori_loop(0, (count + DEPTH - 1) // DEPTH, more, 0)
                ready[turn, half] = total[...].astype(jnp.bfloat16)

            put(window, half).start()
        return carry

    lax.fori_loop(0, bins // ratio, one_window, 0)
    for window in (bins // ratio - 2, bins // ratio - 1):
        for half in range(ratio):
            put(jnp.int32(window), half).wait()


def align(held, rows, ratio, planes, capacity):
    sources, height, length = held.shape
    room = height - META
    deep = -(-(sources * capacity + 2 * STEP) // DEPTH) * DEPTH
    cfg = (sources, room, rows, ratio, planes, deep)
    return pl.pallas_call(
        functools.partial(align_kernel, cfg),
        out_shape=jax.ShapeDtypeStruct((planes, ratio, WINDOWS * length, rows), jnp.bfloat16),
        in_specs=[ANY],
        out_specs=ANY,
        scratch_shapes=[
            pltpu.VMEM((sources * height, length), jnp.bfloat16),
            pltpu.VMEM((2 * sources, LANES), jnp.int32),
            pltpu.SMEM((2 * sources, LANES), jnp.int32),
            pltpu.VMEM((sources * room + 2 * STEP, length), jnp.float32),
            pltpu.VMEM((sources * room + 2 * STEP, LANES), jnp.float32),
            pltpu.VMEM((ratio, deep, length), jnp.float32),
            pltpu.VMEM((ratio, deep, LANES), jnp.float32),
            pltpu.VMEM((length, rows), jnp.float32),
            pltpu.VMEM((2, ratio, length, rows), jnp.bfloat16),
            pltpu.SemaphoreType.DMA((sources + 1,)),
            pltpu.SemaphoreType.DMA((2, ratio)),
        ],
        compiler_params=pltpu.CompilerParams(vmem_limit_bytes=GRANT),
        cost_estimate=pl.CostEstimate(flops=10 * 10**9, bytes_accessed=2 * 10**7, transcendentals=0),
        name="align",
    )(held)


def far_first(planes):
    return [sorted(range(planes), key=lambda p: (-abs(p - z), -p)) for z in range(planes)]


def reduce_kernel(
    cfg, aligned, calib, early, later, out, left, near, far, stage, up, down, kept, total, answer,
    left_sems, near_sems, early_sems, later_sems, far_send, far_recv, up_send, up_recv, down_send, down_recv, out_sems,
):
    planes, ratio, pieces = cfg
    t, c = lax.axis_index("tm"), lax.axis_index("col")
    plane, lot = t // ratio, lax.rem(t, ratio)
    rows = calib.shape[0]
    split = early.shape[1]
    order = far_first(planes)

    def columns(piece):
        return pl.ds(pl.multiple_of(piece * PIECE, PIECE), PIECE)

    def far_copy(step, piece, part):
        place = pl.ds(part * split, split)
        return pltpu.make_async_remote_copy(
            src_ref=calib.at[place, columns(piece)],
            dst_ref=far.at[step - 1, piece, place],
            send_sem=far_send.at[step - 1, piece, part],
            recv_sem=far_recv.at[step - 1, piece, part],
            device_id=(plane * ratio + lax.rem(lot - step + ratio, ratio), c),
            device_id_type=MESH,
        )

    def target(turn):
        return pick(order, plane, turn)

    def near_load(piece):
        return pltpu.make_async_copy(calib.at[:, columns(piece)], near.at[piece], near_sems.at[piece])

    def early_load(step):
        return pltpu.make_async_copy(
            early.at[step - 1], far.at[step - 1, 0, pl.ds(0, split)], early_sems.at[step - 1]
        )

    def later_load(step, piece):
        return pltpu.make_async_copy(
            later.at[step - 1, :, columns(piece)],
            far.at[step - 1, piece, pl.ds(split, split)],
            later_sems.at[step - 1, piece],
        )

    def left_load(turn):
        where = target(turn)
        return pltpu.make_async_copy(aligned.at[where], left.at[where], left_sems.at[turn])

    steps = range(1, ratio)
    opening = [left_load(0), near_load(0)] + [early_load(step) for step in steps] + [later_load(step, 0) for step in steps]
    for load in opening:
        load.start()
    barrier = pltpu.get_barrier_semaphore()
    peers = [(True, (plane * ratio + lax.rem(lot + step, ratio), c)) for step in steps]
    peers += [(plane > 0, (t - ratio, c)), (plane < planes - 1, (t + ratio, c))]
    for near_by, peer in peers:

        @pl.when(near_by)
        def _():
            pl.semaphore_signal(barrier, inc=1, device_id=peer, device_id_type=MESH)

    pl.semaphore_wait(
        barrier, ratio - 1 + jnp.where(plane > 0, 1, 0) + jnp.where(plane < planes - 1, 1, 0)
    )

    late = [(1, 0)] + [(piece, part) for piece in range(2, pieces) for part in range(2)]
    for piece, part in late:
        for step in steps:
            far_copy(step, piece, part).start()
    for load in opening:
        load.wait()
    for turn in range(1, planes):
        left_load(turn).start()
    for piece in range(1, pieces):
        near_load(piece).start()
    for step in steps:
        later_load(step, 1).start()

    def hop(piece, where, buffer, sends, recvs, side):
        return pltpu.make_async_remote_copy(
            src_ref=stage.at[piece, where],
            dst_ref=buffer.at[piece, where],
            send_sem=sends.at[piece, where],
            recv_sem=recvs.at[piece, where],
            device_id=(t + side * ratio, c),
            device_id_type=MESH,
        )

    def go_up(piece, where):
        return hop(piece, where, up, up_send, up_recv, 1)

    def go_down(piece, where):
        return hop(piece, where, down, down_send, down_recv, -1)

    def one_piece(piece, carry):
        @pl.when(piece > 0)
        def _():
            near_load(piece).wait()
            for step in steps:
                far_copy(step, piece, 0).wait_recv()

        @pl.when(piece == 1)
        def _():
            for step in steps:
                later_load(step, 1).wait()

        @pl.when(piece > 1)
        def _():
            for step in steps:
                far_copy(step, piece, 1).wait_recv()

        def one_turn(turn, inner):
            where = target(turn)

            @pl.when((piece == 0) & (turn > 0))
            def _():
                left_load(turn).wait()

            value = jnp.dot(left[where, 0], near[piece], preferred_element_type=jnp.float32)
            for step in range(1, ratio):
                value = value + jnp.dot(
                    left[where, step], far[step - 1, piece], preferred_element_type=jnp.float32
                )
            total[...] = value

            @pl.when((where > plane) & (plane > 0))
            def _():
                go_up(piece, where).wait_recv()
                stage[piece, where] = (total[...] + up[piece, where].astype(jnp.float32)).astype(jnp.bfloat16)

            @pl.when((where < plane) & (plane < planes - 1))
            def _():
                go_down(piece, where).wait_recv()
                stage[piece, where] = (total[...] + down[piece, where].astype(jnp.float32)).astype(jnp.bfloat16)

            @pl.when(((where > plane) & (plane == 0)) | ((where < plane) & (plane == planes - 1)))
            def _():
                stage[piece, where] = total[...].astype(jnp.bfloat16)

            @pl.when(where > plane)
            def _():
                go_up(piece, where).start()

            @pl.when(where < plane)
            def _():
                go_down(piece, where).start()

            @pl.when(where == plane)
            def _():
                kept[piece] = total[...]

            return inner

        lax.fori_loop(0, planes, one_turn, 0)
        return carry

    lax.fori_loop(0, pieces, one_piece, 0)

    def put(piece):
        return pltpu.make_async_copy(
            answer.at[piece],
            out.at[:, pl.ds(pl.multiple_of(piece * PIECE, PIECE), PIECE)],
            out_sems.at[piece],
        )

    def finish(piece, carry):
        @pl.when(plane > 0)
        def _():
            go_up(piece, plane).wait_recv()
            kept[piece] += up[piece, plane].astype(jnp.float32)

        @pl.when(plane < planes - 1)
        def _():
            go_down(piece, plane).wait_recv()
            kept[piece] += down[piece, plane].astype(jnp.float32)

        answer[piece] = kept[piece].astype(jnp.bfloat16)
        put(piece).start()
        return carry

    lax.fori_loop(0, pieces, finish, 0)

    def drain(piece, carry):
        put(piece).wait()
        for where in range(planes):
            @pl.when(where > plane)
            def _():
                go_up(piece, where).wait_send()

            @pl.when(where < plane)
            def _():
                go_down(piece, where).wait_send()

        return carry

    lax.fori_loop(0, pieces, drain, 0)
    for piece, part in late:
        for step in steps:
            far_copy(step, piece, part).wait_send()


def reduce(aligned, calib, early, later):
    planes, ratio, height, rows = aligned.shape
    outputs = calib.shape[1]
    pieces = outputs // PIECE
    cfg = (planes, ratio, pieces)
    far = (ratio - 1, pieces, 2)
    hops = (pieces, planes)
    return pl.pallas_call(
        functools.partial(reduce_kernel, cfg),
        out_shape=jax.ShapeDtypeStruct((height, outputs), jnp.bfloat16),
        in_specs=[ANY] * 4,
        out_specs=ANY,
        scratch_shapes=[
            pltpu.VMEM((planes, ratio, height, rows), jnp.bfloat16),
            pltpu.VMEM((pieces, rows, PIECE), jnp.bfloat16),
            pltpu.VMEM((ratio - 1, pieces, rows, PIECE), jnp.bfloat16),
            pltpu.VMEM((pieces, planes, height, PIECE), jnp.bfloat16),
            pltpu.VMEM((pieces, planes, height, PIECE), jnp.bfloat16),
            pltpu.VMEM((pieces, planes, height, PIECE), jnp.bfloat16),
            pltpu.VMEM((pieces, height, PIECE), jnp.float32),
            pltpu.VMEM((height, PIECE), jnp.float32),
            pltpu.VMEM((pieces, height, PIECE), jnp.bfloat16),
            pltpu.SemaphoreType.DMA((planes,)),
            pltpu.SemaphoreType.DMA((pieces,)),
            pltpu.SemaphoreType.DMA((ratio - 1,)),
            pltpu.SemaphoreType.DMA((ratio - 1, 2)),
            pltpu.SemaphoreType.DMA(far),
            pltpu.SemaphoreType.DMA(far),
            pltpu.SemaphoreType.DMA(hops),
            pltpu.SemaphoreType.DMA(hops),
            pltpu.SemaphoreType.DMA(hops),
            pltpu.SemaphoreType.DMA(hops),
            pltpu.SemaphoreType.DMA((pieces,)),
        ],
        compiler_params=pltpu.CompilerParams(
            collective_id=1, has_side_effects=True, vmem_limit_bytes=GRANT
        ),
        cost_estimate=pl.CostEstimate(flops=20 * 10**9, bytes_accessed=3 * 10**7, transcendentals=0),
        name="reduce",
    )(aligned, calib, early, later)


def per_device(
    block_values, block_shifts, block_sensor, block_window, block_owner, block_counts, calibration
):
    owners = lax.axis_size("tm")
    cols = lax.axis_size("col")
    ratio = owners // cols
    planes = owners // ratio
    rows, outputs = calibration.shape
    blocks = block_values.shape[1]
    capacity = min(blocks, blocks * 3 // (2 * owners))
    def shifted(step):
        return [((t // ratio) * ratio + (t % ratio + step) % ratio, t) for t in range(owners)]

    by_lane = (blocks // LANES, LANES)
    held, early = deliver(
        block_values[0], block_shifts[0], block_sensor.reshape(by_lane), block_window.reshape(by_lane),
        block_owner.reshape(by_lane), block_counts, calibration, owners, cols, capacity,
    )
    part, held = lax.optimization_barrier((calibration[rows // 2:, :2 * PIECE], held))
    later = jnp.stack([lax.ppermute(part, "tm", shifted(step)) for step in range(1, ratio)])
    aligned = align(held, rows, ratio, planes, capacity)
    return reduce(aligned, calibration, early, later)


def solution(mesh):
    placed = (
        P("col", "tm", None),
        P("col", "tm", None),
        P("col", "tm"),
        P("col", "tm"),
        P("col", "tm", None),
        P("col", "tm"),
        P("tm", "col"),
    )
    return jax.shard_map(
        per_device, mesh=mesh, in_specs=placed, out_specs=P("tm", "col"), check_vma=False
    )
```

```python
import functools

import jax
import jax.numpy as jnp
from jax import lax
from jax.experimental import pallas as pl
from jax.experimental.pallas import tpu as pltpu
from jax.sharding import PartitionSpec as P

WINDOWS = 4
LANES = 128
META = 32
DEPTH = 256
STEP = 64
WIDTH = 1024
PARTS = 2
PIECE = 256
GRANT = 67_000_000


ANY = pl.BlockSpec(memory_space=pl.ANY)
VMEM = pl.BlockSpec(memory_space=pltpu.VMEM)
MESH = pl.DeviceIdType.MESH


def cut(whole, size):
    return jnp.floor((whole + 0.5) * (1.0 / size))


def near_first(groups):
    return [sorted(range(groups), key=lambda g: (abs(g - me), g)) for me in range(groups)]


def pick(table, mine, turn):
    chosen = jnp.int32(0)
    for own, row in enumerate(table):
        value = jnp.int32(0)
        for at, entry in enumerate(row):
            value = value + jnp.where(turn == at, entry, 0)
        chosen = chosen + jnp.where(mine == own, value, 0)
    return chosen


def spread_rows(values, shifts):
    samples = values.astype(jnp.float32)
    offsets = shifts.astype(jnp.float32)
    lane = lax.broadcasted_iota(jnp.int32, samples.shape, 1)
    result = None
    for displace in (-1, 0, 1):
        weight = jnp.maximum(0.0, 1.0 - jnp.abs(offsets - displace)).astype(jnp.bfloat16)
        product = weight.astype(jnp.float32) * samples
        if displace == 1:
            product = jnp.where(lane == 0, 0.0, pltpu.roll(product, 1, 1))
        elif displace == -1:
            product = jnp.where(lane == LANES - 1, 0.0, pltpu.roll(product, LANES - 1, 1))
        result = product if result is None else result + product
    return result


def sort_blocks(cfg, values, shifts, sensor, window, owner, count, parcel, payload, bases, tops, notes, send):
    owners, cols, rows, room = cfg
    ratio = owners // cols
    planes = owners // ratio
    groups = sensor.shape[0]
    shares = ratio * rows // WIDTH
    bins = planes * WINDOWS * shares
    every = ratio * bins
    third = room // LANES
    lane = lax.broadcasted_iota(jnp.int32, (1, LANES), 1).astype(jnp.float32)
    down = lax.broadcasted_iota(jnp.int32, (LANES, LANES), 0).astype(jnp.float32)
    index = (
        lax.broadcasted_iota(jnp.int32, (groups, LANES), 0) * LANES
        + lax.broadcasted_iota(jnp.int32, (groups, LANES), 1)
    )
    live = index < count[...]
    who = owner[...].astype(jnp.float32)
    what = sensor[...].astype(jnp.float32)
    where = cut(who, ratio)
    share = cut(what, WIDTH)
    number = (where * WINDOWS + window[...].astype(jnp.float32)) * shares + share
    number = jnp.where(live, (who - ratio * where) * bins + number, -1.0)
    local = what - WIDTH * share
    local_top = cut(local, LANES)
    local_low = local - LANES * local_top
    bin_row = lax.broadcasted_iota(jnp.int32, (every, LANES), 0).astype(jnp.float32)
    hot = [jnp.where(number[r:r + 1] == bin_row, 1.0, 0.0) for r in range(groups)]
    before = jnp.concatenate([jnp.where(down < lane, 1.0, 0.0), jnp.ones((LANES, LANES), jnp.float32)], axis=1)
    earlier = jnp.dot(
        jnp.concatenate(hot, axis=0).astype(jnp.bfloat16), before.astype(jnp.bfloat16),
        preferred_element_type=jnp.float32,
    )
    run = jnp.zeros((every, LANES), jnp.float32)
    offset = []
    for r in range(groups):
        part = earlier[r * every:(r + 1) * every]
        offset.append(run + part[:, :LANES])
        run = run + part[:, LANES:]
    upto = run
    shift = 1
    while shift < every:
        upto = upto + jnp.where(bin_row >= shift, pltpu.roll(upto, shift, 0), 0.0)
        shift *= 2
    begin = upto - run
    begin = jnp.concatenate(
        [begin[p * bins:(p + 1) * bins] - begin[p * bins:p * bins + 1] for p in range(ratio)], axis=0
    )
    end = begin + run
    lot_of = cut(bin_row, bins)
    first = begin + lot_of * room
    for r in range(groups):
        spot = jnp.sum(hot[r] * (first + offset[r]), axis=0, keepdims=True)
        spot = jnp.where(live[r:r + 1], spot, -1.0)
        top = cut(jnp.maximum(spot, 0.0), LANES)
        tops[r:r + 1, :] = jnp.where(spot < 0.0, -1.0, top)
        bases[:, r * LANES:(r + 1) * LANES] = jnp.where(spot - top * LANES == down, 1.0, 0.0).astype(jnp.bfloat16)
        at = pl.ds(r * LANES, LANES)
        payload[at, :LANES] = spread_rows(values[at, :], shifts[at, :]).astype(jnp.bfloat16)
        tag = jnp.where(
            down < LANES // 2,
            jnp.broadcast_to(local_top[r:r + 1], (LANES, LANES)),
            jnp.broadcast_to(local_low[r:r + 1], (LANES, LANES)),
        )
        payload[at, LANES:] = jnp.transpose(tag).astype(jnp.bfloat16)
    edge = []
    for column in (begin, end):
        if every < LANES:
            column = jnp.concatenate([column, jnp.zeros((LANES - every, LANES), jnp.float32)], axis=0)
        row = jnp.transpose(column)[0:1]
        high = cut(row, 64)
        edge += [high, row - 64 * high]
    notes[...] = jnp.zeros_like(notes)
    for p in range(ratio):
        for k, row in enumerate(edge):
            notes[p, 2 * third + k:2 * third + k + 1, :] = row
    tile = 4 * LANES
    for p in range(ratio):

        def one_tile(step, carry, p=p):
            strips = []
            for k in range(tile // LANES):
                wanted = (step * (tile // LANES) + k + p * third).astype(jnp.float32)
                chosen = jnp.where(tops[...] == wanted, 1.0, 0.0).astype(jnp.bfloat16)
                strips.append(
                    jnp.concatenate(
                        [bases[:, r * LANES:(r + 1) * LANES] * chosen[r:r + 1] for r in range(groups)], axis=1
                    )
                )
            placed = jnp.dot(jnp.concatenate(strips, axis=0), payload[...], preferred_element_type=jnp.float32)
            parcel[p, pl.ds(pl.multiple_of(step * tile, tile), tile), :] = placed[:, :LANES].astype(jnp.bfloat16)
            for k in range(tile // LANES):
                flat = jnp.transpose(placed[k * LANES:(k + 1) * LANES, LANES:])
                at = step * (tile // LANES) + k
                notes[p, pl.ds(at, 1), :] = flat[0:1]
                notes[p, pl.ds(third + at, 1), :] = flat[LANES // 2:LANES // 2 + 1]
            return carry

        lax.fori_loop(0, room // tile, one_tile, 0)
        parcel[p, room:room + META, :] = notes[p].astype(jnp.bfloat16)
        send(p)


def greet(peers):
    barrier = pltpu.get_barrier_semaphore()
    for peer in peers:
        pl.semaphore_signal(barrier, inc=1, device_id=peer, device_id_type=MESH)
    pl.semaphore_wait(barrier, len(peers))


def deliver_kernel(
    cfg, values_in, shifts_in, sensor_in, window_in, owner_in, count, calib, held, early, part,
    bridge, bridge_sems, values, shifts, sensor, window, owner, load_sems, parcel, relay, payload, bases, tops, notes, send_sems, recv_sems, relay_send, relay_recv, turn_sems,
    side_sems, pass_sems, own_sems, far_send, far_recv,
):
    owners, cols, rows, room = cfg
    ratio = owners // cols
    planes = owners // ratio
    chips = cols // 2
    t, c = lax.axis_index("tm"), lax.axis_index("col")
    core, chip = lax.rem(c, 2), c // 2
    plane, lot = t // ratio, lax.rem(t, ratio)
    first = core == lax.rem(plane, 2)

    def line_of(source, column):
        return lax.rem(source // ratio + lax.rem(source, ratio) + column, chips)

    line = line_of(t, c)
    quarter = rows // 4

    def far_copy(step, turn):
        place = pl.ds(turn * quarter, quarter if turn == 0 else rows - quarter)
        return pltpu.make_async_remote_copy(
            src_ref=calib.at[place, pl.ds(0, PIECE)],
            dst_ref=early.at[step - 1, place],
            send_sem=far_send.at[step - 1, turn],
            recv_sem=far_recv.at[step - 1, turn],
            device_id=(plane * ratio + lax.rem(lot - step + ratio, ratio), c),
            device_id_type=MESH,
        )

    def part_of(k):
        size = (room + META) // PARTS
        return pl.ds(k * size, size)

    def own_copy(origin, source, from_lot, k):
        return pltpu.make_async_copy(
            origin.at[part_of(k)], held.at[source, part_of(k)], own_sems.at[from_lot, k]
        )

    def out_copy(target, k):
        return pltpu.make_async_remote_copy(
            src_ref=parcel.at[target, part_of(k)],
            dst_ref=held.at[t, part_of(k)],
            send_sem=send_sems.at[target, k],
            recv_sem=recv_sems.at[t, k],
            device_id=(c * ratio + target, c),
            device_id_type=MESH,
        )

    def relay_copy(target, k):
        return pltpu.make_async_remote_copy(
            src_ref=parcel.at[target, part_of(k)],
            dst_ref=relay.at[lot, chip, part_of(k)],
            send_sem=relay_send.at[target, k],
            recv_sem=relay_recv.at[lot, chip, k],
            device_id=(plane * ratio + target, line * 2 + core),
            device_id_type=MESH,
        )

    def relay_arrival(from_lot, from_chip, k):
        return pltpu.make_async_remote_copy(
            src_ref=parcel.at[0, part_of(k)],
            dst_ref=relay.at[from_lot, from_chip, part_of(k)],
            send_sem=relay_send.at[0, k],
            recv_sem=relay_recv.at[from_lot, from_chip, k],
            device_id=(plane * ratio + from_lot, from_chip * 2 + core),
            device_id_type=MESH,
        )

    def turn_copy(from_lot, from_chip, k):
        source = plane * ratio + from_lot
        return pltpu.make_async_remote_copy(
            src_ref=relay.at[from_lot, from_chip, part_of(k)],
            dst_ref=held.at[source, part_of(k)],
            send_sem=turn_sems.at[from_lot, from_chip, k],
            recv_sem=recv_sems.at[source, k],
            device_id=((from_chip * 2 + core) * ratio + lot, c),
            device_id_type=MESH,
        )

    def pass_copy(source, k):
        return pltpu.make_async_remote_copy(
            src_ref=held.at[source, part_of(k)],
            dst_ref=held.at[source, part_of(k)],
            send_sem=pass_sems.at[source, k],
            recv_sem=recv_sems.at[source, k],
            device_id=(t, c + 1 - 2 * core),
            device_id_type=MESH,
        )

    def side_copy(source, step, k):
        return pltpu.make_async_remote_copy(
            src_ref=held.at[source, part_of(k)],
            dst_ref=held.at[source, part_of(k)],
            send_sem=side_sems.at[step - 1, source, k],
            recv_sem=recv_sems.at[source, k],
            device_id=(t, lax.rem(chip + step, chips) * 2 + core),
            device_id_type=MESH,
        )

    loads = [
        pltpu.make_async_copy(source, target, load_sems.at[k])
        for k, (source, target) in enumerate(
            ((owner_in, owner), (sensor_in, sensor), (window_in, window), (values_in, values), (shifts_in, shifts))
        )
    ]
    for load in loads:
        load.start()
    bridge_in = pltpu.make_async_copy(
        calib.at[pl.ds(rows // 4, rows - rows // 4), pl.ds(PIECE, PIECE)], bridge, bridge_sems.at[0]
    )
    bridge_out = pltpu.make_async_copy(bridge, part, bridge_sems.at[1])
    bridge_in.start()
    greet(
        [(lax.rem(t + step, owners), c) for step in range(1, owners)]
        + [
            (plane * ratio + lax.rem(lot + side, ratio), lax.rem(c + step, cols))
            for side in range(ratio)
            for step in range(1, cols)
        ]
    )
    for step in range(1, ratio):
        far_copy(step, 0).start()
    for load in loads:
        load.wait()

    def send(target):
        straight = (line == chip) & (target == lot)

        @pl.when(jnp.logical_not(straight))
        def _():
            for k in range(PARTS):
                relay_copy(target, k).start()

        @pl.when(straight & (plane == c))
        def _():
            for k in range(PARTS):
                own_copy(parcel.at[target], t, lot, k).start()

        @pl.when(straight & (plane != c))
        def _():
            for k in range(PARTS):
                out_copy(target, k).start()

    sort_blocks(
        cfg, values, shifts, sensor, window, owner, count, parcel, payload, bases, tops, notes, send
    )

    bridge_in.wait()
    bridge_out.start()

    for step in range(1, ratio):
        far_copy(step, 1).start()

    def each_turn(act):
        for k in range(PARTS):
            for side in range(ratio):
                for step in range(chips):
                    if side or step:
                        from_lot, from_chip = lax.rem(lot + side, ratio), lax.rem(chip + step, chips)
                        column = from_chip * 2 + core

                        @pl.when(line_of(plane * ratio + from_lot, column) == chip)
                        def _():
                            act(from_lot, from_chip, k, column == plane)

    def forward(from_lot, from_chip, k, here):
        relay_arrival(from_lot, from_chip, k).wait_recv()

        @pl.when(here)
        def _():
            own_copy(relay.at[from_lot, from_chip], plane * ratio + from_lot, from_lot, k).start()

        @pl.when(jnp.logical_not(here))
        def _():
            turn_copy(from_lot, from_chip, k).start()

    each_turn(forward)
    table = near_first(planes)
    nearest = [
        (pick(table, plane, turn) * ratio + lax.rem(lot + step, ratio), k)
        for turn in range(planes)
        for step in range(ratio)
        for k in range(PARTS)
    ]

    for source, k in nearest:
        entry = first & (line_of(source, plane) == chip)

        @pl.when(entry & (source // ratio == plane))
        def _():
            own_copy(parcel.at[0], source, lax.rem(source, ratio), k).wait()

        @pl.when(entry & (source // ratio != plane))
        def _():
            pass_copy(source, k).wait_recv()

        @pl.when(entry)
        def _():
            for step in range(1, chips):
                side_copy(source, step, k).start()
            pass_copy(source, k).start()

    for source, k in nearest:

        @pl.when(first & (line_of(source, plane) != chip))
        def _():
            pass_copy(source, k).wait_recv()
            pass_copy(source, k).start()

    for target in range(ratio):
        straight = (line == chip) & (target == lot)

        @pl.when(straight & (plane != c))
        def _():
            for k in range(PARTS):
                out_copy(target, k).wait_send()

        @pl.when(jnp.logical_not(straight))
        def _():
            for k in range(PARTS):
                relay_copy(target, k).wait_send()

    def settle(from_lot, from_chip, k, here):
        @pl.when(jnp.logical_not(here))
        def _():
            turn_copy(from_lot, from_chip, k).wait_send()

    each_turn(settle)

    for source in range(owners):
        for k in range(PARTS):

            @pl.when(first & (line_of(source, plane) == chip))
            def _():
                for step in range(1, chips):
                    side_copy(source, step, k).wait_send()

            @pl.when(first)
            def _():
                pass_copy(source, k).wait_send()

            @pl.when(jnp.logical_not(first))
            def _():
                pass_copy(source, k).wait_recv()

    for step in range(1, ratio):
        for turn in range(2):
            far_copy(step, turn).wait()
    bridge_out.wait()


def deliver(values, shifts, sensor, window, owner, count, calib, owners, cols, capacity):
    ratio = owners // cols
    blocks, length = values.shape
    rows = calib.shape[0]
    room = owners // ratio * capacity
    every = owners * WINDOWS * ratio
    chips = cols // 2
    cfg = (owners, cols, rows, room)
    groups = blocks // LANES
    return pl.pallas_call(
        functools.partial(deliver_kernel, cfg),
        out_shape=[
            jax.ShapeDtypeStruct((owners, room + META, length), jnp.bfloat16),
            jax.ShapeDtypeStruct((ratio - 1, rows, PIECE), jnp.bfloat16),
            jax.ShapeDtypeStruct((rows - rows // 4, PIECE), jnp.bfloat16),
        ],
        in_specs=[ANY] * 5 + [VMEM, ANY],
        out_specs=[ANY] * 3,
        scratch_shapes=[
            pltpu.VMEM((rows - rows // 4, PIECE), jnp.bfloat16),
            pltpu.SemaphoreType.DMA((2,)),
            pltpu.VMEM((blocks, length), jnp.bfloat16),
            pltpu.VMEM((blocks, length), jnp.bfloat16),
            pltpu.VMEM((groups, LANES), jnp.int32),
            pltpu.VMEM((groups, LANES), jnp.int32),
            pltpu.VMEM((groups, LANES), jnp.int32),
            pltpu.SemaphoreType.DMA((5,)),
            pltpu.VMEM((ratio, room + META, length), jnp.bfloat16),
            pltpu.VMEM((ratio, chips, room + META, length), jnp.bfloat16),
            pltpu.VMEM((blocks, 2 * LANES), jnp.bfloat16),
            pltpu.VMEM((LANES, blocks), jnp.bfloat16),
            pltpu.VMEM((groups, LANES), jnp.float32),
            pltpu.VMEM((ratio, META, LANES), jnp.float32),
            pltpu.SemaphoreType.DMA((ratio, PARTS)),
            pltpu.SemaphoreType.DMA((owners, PARTS)),
            pltpu.SemaphoreType.DMA((ratio, PARTS)),
            pltpu.SemaphoreType.DMA((ratio, chips, PARTS)),
            pltpu.SemaphoreType.DMA((ratio, chips, PARTS)),
            pltpu.SemaphoreType.DMA((max(chips - 1, 1), owners, PARTS)),
            pltpu.SemaphoreType.DMA((owners, PARTS)),
            pltpu.SemaphoreType.DMA((ratio, PARTS)),
            pltpu.SemaphoreType.DMA((ratio - 1, 2)),
            pltpu.SemaphoreType.DMA((ratio - 1, 2)),
        ],
        compiler_params=pltpu.CompilerParams(
            collective_id=0, has_side_effects=True, vmem_limit_bytes=GRANT
        ),
        cost_estimate=pl.CostEstimate(flops=10 * 10**9, bytes_accessed=10**7, transcendentals=0),
        name="deliver",
    )(values, shifts, sensor, window, owner, count, calib)


def align_kernel(cfg, held, aligned, raw, limit, limit_s, contrib, names, stage, tags, total, ready, sems, out_sems):
    sources, room, rows, ratio, planes, deep = cfg
    shares = ratio * rows // WIDTH
    bins = planes * WINDOWS * shares
    lot = lax.rem(lax.axis_index("tm"), ratio)
    height = room + META
    third = room // LANES
    loads = [
        pltpu.make_async_copy(held.at[s], raw.at[pl.ds(s * height, height)], sems.at[s])
        for s in range(sources)
    ]
    for load in loads:
        load.start()
    stage[...] = jnp.zeros_like(stage)
    tags[...] = jnp.zeros_like(tags)
    tail = pl.ds(sources * room, contrib.shape[0] - sources * room)
    contrib[tail, :] = jnp.zeros_like(contrib[tail, :])
    names[tail, :] = jnp.zeros_like(names[tail, :])
    for s in range(sources):
        loads[s].wait()
        meta = raw[pl.ds(s * height + room, META), :].astype(jnp.float32)
        for side in range(2):
            at = 2 * third + 2 * side
            limit[pl.ds(side * sources + s, 1), :] = (
                meta[at:at + 1] * 64.0 + meta[at + 1:at + 2]
            ).astype(jnp.int32)
        for r in range(third):
            tag = meta[r:r + 1] * float(LANES) + meta[third + r:third + r + 1]
            at = pl.ds(s * room + r * LANES, LANES)
            names[at, :] = jnp.transpose(jnp.broadcast_to(tag, (LANES, LANES)))
            contrib[at, :] = raw[pl.ds(s * height + r * LANES, LANES), :].astype(jnp.float32)
    fetch = pltpu.make_async_copy(limit, limit_s, sems.at[sources])
    fetch.start()
    fetch.wait()
    def put(window, half):
        turn = lax.rem(window, 2)
        return pltpu.make_async_copy(
            ready.at[turn, half],
            aligned.at[
                window // WINDOWS,
                lax.rem(half - lot + ratio, ratio),
                pl.ds(pl.multiple_of(lax.rem(window, WINDOWS) * LANES, LANES), LANES),
            ],
            out_sems.at[turn, half],
        )

    def copy_rows(source, target, share, extent):
        stage[share, pl.ds(target, extent), :] = contrib[pl.ds(source, extent), :]
        tags[share, pl.ds(target, extent), :] = names[pl.ds(source, extent), :]

    def chunk(share, at, size, count, write):
        place = pl.ds(pl.multiple_of(at * size, size), size)
        left = jnp.transpose(stage[share, place, :]).astype(jnp.bfloat16)
        tag = tags[share, place, :]
        top = jnp.floor(tag * (1.0 / LANES))
        low = tag - top * LANES
        lane = lax.broadcasted_iota(jnp.int32, (size, LANES), 1).astype(jnp.float32)
        row = lax.broadcasted_iota(jnp.int32, (size, LANES), 0)
        base = jnp.where((low == lane) & (row + at * size < count), 1.0, 0.0).astype(jnp.bfloat16)
        top = top.astype(jnp.bfloat16)
        nothing = jnp.zeros_like(base)
        wide = 4 * LANES
        for n in range(WIDTH // wide):
            hot = jnp.concatenate(
                [
                    jnp.where(top == jnp.bfloat16(n * (wide // LANES) + k), base, nothing)
                    for k in range(wide // LANES)
                ],
                axis=1,
            )
            write(n * wide, wide, jnp.dot(left, hot, preferred_element_type=jnp.float32))

    def one_window(window, carry):
        turn = lax.rem(window, 2)

        @pl.when(window >= 2)
        def _():
            for half in range(ratio):
                put(window - 2, half).wait()

        spans, counts = [], []
        longest, largest = 0, 0
        for share in range(shares):
            number = lot * bins + window * shares + share
            count = 0
            for s in range(sources):
                begin = limit_s[s, number]
                extent = limit_s[sources + s, number] - begin
                spans.append((share, s * room + begin, count, extent))
                count = count + extent
                longest = jnp.maximum(longest, extent)
            counts.append(count)
            largest = jnp.maximum(largest, count)

        for low, high in ((-1, STEP // 4), (STEP // 4, STEP // 2), (STEP // 2, STEP)):

            @pl.when((longest > low) & (longest <= high))
            def _():
                for share, source, target, _ in spans:
                    copy_rows(source, target, share, high)

        @pl.when(longest > STEP)
        def _():
            for share, source, target, extent in spans:

                def more(step, inner, share=share, source=source, target=target):
                    copy_rows(source + step * STEP, target + step * STEP, share, STEP)
                    return inner

                lax.fori_loop(0, (extent + STEP - 1) // STEP, more, 0)

        def spot(share, start, size):
            place = share * WIDTH
            return turn, place // rows, slice(None), pl.ds(place % rows + start, size)

        def whole(size):
            for share in range(shares):

                def store(start, extent, value, share=share):
                    ready[spot(share, start, extent)] = value.astype(jnp.bfloat16)

                chunk(share, 0, size, counts[share], store)

        @pl.when(largest <= DEPTH)
        def _():
            whole(DEPTH)

        @pl.when((largest > DEPTH) & (largest <= 2 * DEPTH))
        def _():
            whole(2 * DEPTH)

        @pl.when(largest > 2 * DEPTH)
        def _():
            for share in range(shares):
                total[...] = jnp.zeros_like(total)

                def add(start, extent, value):
                    total[:, pl.ds(start, extent)] += value

                def more(at, inner, share=share):
                    chunk(share, at, DEPTH, counts[share], add)
                    return inner

                lax.fori_loop(0, (counts[share] + DEPTH - 1) // DEPTH, more, 0)
                ready[spot(share, 0, WIDTH)] = total[...].astype(jnp.bfloat16)

        for half in range(ratio):
            put(window, half).start()
        return carry

    lax.fori_loop(0, planes * WINDOWS, one_window, 0)
    for window in (planes * WINDOWS - 2, planes * WINDOWS - 1):
        for half in range(ratio):
            put(jnp.int32(window), half).wait()


def align(held, rows, ratio, planes, capacity):
    sources, height, length = held.shape
    room = height - META
    deep = -(-(sources * capacity + 2 * STEP) // DEPTH) * DEPTH
    cfg = (sources, room, rows, ratio, planes, deep)
    return pl.pallas_call(
        functools.partial(align_kernel, cfg),
        out_shape=jax.ShapeDtypeStruct((planes, ratio, WINDOWS * length, rows), jnp.bfloat16),
        in_specs=[ANY],
        out_specs=ANY,
        scratch_shapes=[
            pltpu.VMEM((sources * height, length), jnp.bfloat16),
            pltpu.VMEM((2 * sources, LANES), jnp.int32),
            pltpu.SMEM((2 * sources, LANES), jnp.int32),
            pltpu.VMEM((sources * room + 2 * STEP, length), jnp.float32),
            pltpu.VMEM((sources * room + 2 * STEP, LANES), jnp.float32),
            pltpu.VMEM((ratio * rows // WIDTH, deep, length), jnp.float32),
            pltpu.VMEM((ratio * rows // WIDTH, deep, LANES), jnp.float32),
            pltpu.VMEM((length, WIDTH), jnp.float32),
            pltpu.VMEM((2, ratio, length, rows), jnp.bfloat16),
            pltpu.SemaphoreType.DMA((sources + 1,)),
            pltpu.SemaphoreType.DMA((2, ratio)),
        ],
        compiler_params=pltpu.CompilerParams(vmem_limit_bytes=GRANT),
        cost_estimate=pl.CostEstimate(flops=10 * 10**9, bytes_accessed=2 * 10**7, transcendentals=0),
        name="align",
    )(held)


def far_first(planes):
    return [sorted(range(planes), key=lambda p: (-abs(p - z), -p)) for z in range(planes)]


def reduce_kernel(
    cfg, aligned, calib, early, later, out, left, near, far, stage, up, down, kept, total, answer,
    left_sems, near_sems, early_sems, later_sems, far_send, far_recv, up_send, up_recv, down_send, down_recv, out_sems,
):
    planes, ratio, pieces = cfg
    t, c = lax.axis_index("tm"), lax.axis_index("col")
    plane, lot = t // ratio, lax.rem(t, ratio)
    rows = calib.shape[0]
    gap = rows - later.shape[1]
    split = rows // 2
    order = far_first(planes)

    def columns(piece):
        return pl.ds(pl.multiple_of(piece * PIECE, PIECE), PIECE)

    def far_copy(step, piece, part):
        place = pl.ds(0, gap) if part == 2 else pl.ds(part * split, split)
        return pltpu.make_async_remote_copy(
            src_ref=calib.at[place, columns(piece)],
            dst_ref=far.at[step - 1, piece, place],
            send_sem=far_send.at[step - 1, piece, part],
            recv_sem=far_recv.at[step - 1, piece, part],
            device_id=(plane * ratio + lax.rem(lot - step + ratio, ratio), c),
            device_id_type=MESH,
        )

    def target(turn):
        return pick(order, plane, turn)

    def near_load(piece):
        return pltpu.make_async_copy(calib.at[:, columns(piece)], near.at[piece], near_sems.at[piece])

    def early_load(step):
        return pltpu.make_async_copy(
            early.at[step - 1], far.at[step - 1, 0], early_sems.at[step - 1]
        )

    def later_load(step):
        return pltpu.make_async_copy(
            later.at[step - 1], far.at[step - 1, 1, pl.ds(gap, rows - gap)], later_sems.at[step - 1]
        )

    def left_load(turn):
        where = target(turn)
        return pltpu.make_async_copy(aligned.at[where], left.at[where], left_sems.at[turn])

    steps = range(1, ratio)
    opening = [left_load(0), near_load(0)] + [early_load(step) for step in steps]
    for load in opening:
        load.start()
    barrier = pltpu.get_barrier_semaphore()
    peers = [(True, (plane * ratio + lax.rem(lot + step, ratio), c)) for step in steps]
    peers += [(plane > 0, (t - ratio, c)), (plane < planes - 1, (t + ratio, c))]
    for near_by, peer in peers:

        @pl.when(near_by)
        def _():
            pl.semaphore_signal(barrier, inc=1, device_id=peer, device_id_type=MESH)

    pl.semaphore_wait(
        barrier, ratio - 1 + jnp.where(plane > 0, 1, 0) + jnp.where(plane < planes - 1, 1, 0)
    )

    late = [(1, 2)] + [(piece, part) for piece in range(2, pieces) for part in range(2)]
    for piece, part in late:
        for step in steps:
            far_copy(step, piece, part).start()
    for load in opening:
        load.wait()
    for turn in range(1, planes):
        left_load(turn).start()
    for piece in range(1, pieces):
        near_load(piece).start()
    for step in steps:
        later_load(step).start()

    def hop(piece, where, buffer, sends, recvs, side):
        return pltpu.make_async_remote_copy(
            src_ref=stage.at[piece, where],
            dst_ref=buffer.at[piece, where],
            send_sem=sends.at[piece, where],
            recv_sem=recvs.at[piece, where],
            device_id=(t + side * ratio, c),
            device_id_type=MESH,
        )

    def go_up(piece, where):
        return hop(piece, where, up, up_send, up_recv, 1)

    def go_down(piece, where):
        return hop(piece, where, down, down_send, down_recv, -1)

    def one_piece(piece, carry):
        @pl.when(piece > 0)
        def _():
            near_load(piece).wait()

        @pl.when(piece == 1)
        def _():
            for step in steps:
                later_load(step).wait()
                far_copy(step, 1, 2).wait_recv()

        @pl.when(piece > 1)
        def _():
            for step in steps:
                for part in range(2):
                    far_copy(step, piece, part).wait_recv()

        def one_turn(turn, inner):
            where = target(turn)

            @pl.when((piece == 0) & (turn > 0))
            def _():
                left_load(turn).wait()

            value = jnp.dot(left[where, 0], near[piece], preferred_element_type=jnp.float32)
            for step in range(1, ratio):
                value = value + jnp.dot(
                    left[where, step], far[step - 1, piece], preferred_element_type=jnp.float32
                )
            total[...] = value

            @pl.when((where > plane) & (plane > 0))
            def _():
                go_up(piece, where).wait_recv()
                stage[piece, where] = (total[...] + up[piece, where].astype(jnp.float32)).astype(jnp.bfloat16)

            @pl.when((where < plane) & (plane < planes - 1))
            def _():
                go_down(piece, where).wait_recv()
                stage[piece, where] = (total[...] + down[piece, where].astype(jnp.float32)).astype(jnp.bfloat16)

            @pl.when(((where > plane) & (plane == 0)) | ((where < plane) & (plane == planes - 1)))
            def _():
                stage[piece, where] = total[...].astype(jnp.bfloat16)

            @pl.when(where > plane)
            def _():
                go_up(piece, where).start()

            @pl.when(where < plane)
            def _():
                go_down(piece, where).start()

            @pl.when(where == plane)
            def _():
                kept[piece] = total[...]

            return inner

        lax.fori_loop(0, planes, one_turn, 0)
        return carry

    lax.fori_loop(0, pieces, one_piece, 0)

    def put(piece):
        return pltpu.make_async_copy(
            answer.at[piece],
            out.at[:, pl.ds(pl.multiple_of(piece * PIECE, PIECE), PIECE)],
            out_sems.at[piece],
        )

    def finish(piece, carry):
        @pl.when(plane > 0)
        def _():
            go_up(piece, plane).wait_recv()
            kept[piece] += up[piece, plane].astype(jnp.float32)

        @pl.when(plane < planes - 1)
        def _():
            go_down(piece, plane).wait_recv()
            kept[piece] += down[piece, plane].astype(jnp.float32)

        answer[piece] = kept[piece].astype(jnp.bfloat16)
        put(piece).start()
        return carry

    lax.fori_loop(0, pieces, finish, 0)

    def drain(piece, carry):
        put(piece).wait()
        for where in range(planes):
            @pl.when(where > plane)
            def _():
                go_up(piece, where).wait_send()

            @pl.when(where < plane)
            def _():
                go_down(piece, where).wait_send()

        return carry

    lax.fori_loop(0, pieces, drain, 0)
    for piece, part in late:
        for step in steps:
            far_copy(step, piece, part).wait_send()


def reduce(aligned, calib, early, later):
    planes, ratio, height, rows = aligned.shape
    outputs = calib.shape[1]
    pieces = outputs // PIECE
    cfg = (planes, ratio, pieces)
    far = (ratio - 1, pieces, 3)
    hops = (pieces, planes)
    return pl.pallas_call(
        functools.partial(reduce_kernel, cfg),
        out_shape=jax.ShapeDtypeStruct((height, outputs), jnp.bfloat16),
        in_specs=[ANY] * 4,
        out_specs=ANY,
        scratch_shapes=[
            pltpu.VMEM((planes, ratio, height, rows), jnp.bfloat16),
            pltpu.VMEM((pieces, rows, PIECE), jnp.bfloat16),
            pltpu.VMEM((ratio - 1, pieces, rows, PIECE), jnp.bfloat16),
            pltpu.VMEM((pieces, planes, height, PIECE), jnp.bfloat16),
            pltpu.VMEM((pieces, planes, height, PIECE), jnp.bfloat16),
            pltpu.VMEM((pieces, planes, height, PIECE), jnp.bfloat16),
            pltpu.VMEM((pieces, height, PIECE), jnp.float32),
            pltpu.VMEM((height, PIECE), jnp.float32),
            pltpu.VMEM((pieces, height, PIECE), jnp.bfloat16),
            pltpu.SemaphoreType.DMA((planes,)),
            pltpu.SemaphoreType.DMA((pieces,)),
            pltpu.SemaphoreType.DMA((ratio - 1,)),
            pltpu.SemaphoreType.DMA((ratio - 1,)),
            pltpu.SemaphoreType.DMA(far),
            pltpu.SemaphoreType.DMA(far),
            pltpu.SemaphoreType.DMA(hops),
            pltpu.SemaphoreType.DMA(hops),
            pltpu.SemaphoreType.DMA(hops),
            pltpu.SemaphoreType.DMA(hops),
            pltpu.SemaphoreType.DMA((pieces,)),
        ],
        compiler_params=pltpu.CompilerParams(
            collective_id=1, has_side_effects=True, vmem_limit_bytes=GRANT
        ),
        cost_estimate=pl.CostEstimate(flops=20 * 10**9, bytes_accessed=3 * 10**7, transcendentals=0),
        name="reduce",
    )(aligned, calib, early, later)


def per_device(
    block_values, block_shifts, block_sensor, block_window, block_owner, block_counts, calibration
):
    owners = lax.axis_size("tm")
    cols = lax.axis_size("col")
    ratio = owners // cols
    planes = owners // ratio
    rows, outputs = calibration.shape
    blocks = block_values.shape[1]
    capacity = min(blocks, blocks * 3 // (2 * owners))
    def shifted(step):
        return [((t // ratio) * ratio + (t % ratio + step) % ratio, t) for t in range(owners)]

    by_lane = (blocks // LANES, LANES)
    held, early, part = deliver(
        block_values[0], block_shifts[0], block_sensor.reshape(by_lane), block_window.reshape(by_lane),
        block_owner.reshape(by_lane), block_counts, calibration, owners, cols, capacity,
    )
    later = jnp.stack([lax.ppermute(part, "tm", shifted(step)) for step in range(1, ratio)])
    aligned = align(held, rows, ratio, planes, capacity)
    return reduce(aligned, calibration, early, later)


def solution(mesh):
    placed = (
        P("col", "tm", None),
        P("col", "tm", None),
        P("col", "tm"),
        P("col", "tm"),
        P("col", "tm", None),
        P("col", "tm"),
        P("tm", "col"),
    )
    return jax.shard_map(
        per_device, mesh=mesh, in_specs=placed, out_specs=P("tm", "col"), check_vma=False
    )
```

```python
import functools

import jax
import jax.numpy as jnp
from jax import lax
from jax.experimental import pallas as pl
from jax.experimental.pallas import tpu as pltpu
from jax.sharding import PartitionSpec as P

WINDOWS = 4
LANES = 128
META = 64
DEPTH = 256
STEP = 48
WIDTH = 1024
PARTS = 4
PIECE = 256
GRANT = 67_000_000


ANY = pl.BlockSpec(memory_space=pl.ANY)
VMEM = pl.BlockSpec(memory_space=pltpu.VMEM)
MESH = pl.DeviceIdType.MESH


def cut(whole, size):
    return jnp.floor((whole + 0.5) * (1.0 / size))


def near_first(groups):
    return [sorted(range(groups), key=lambda g: (abs(g - me), g)) for me in range(groups)]


def pick(table, mine, turn):
    chosen = jnp.int32(0)
    for own, row in enumerate(table):
        value = jnp.int32(0)
        for at, entry in enumerate(row):
            value = value + jnp.where(turn == at, entry, 0)
        chosen = chosen + jnp.where(mine == own, value, 0)
    return chosen


def spread_rows(values, shifts):
    samples = values.astype(jnp.float32)
    offsets = shifts.astype(jnp.float32)
    lane = lax.broadcasted_iota(jnp.int32, samples.shape, 1)
    result = None
    for displace in (-1, 0, 1):
        weight = jnp.maximum(0.0, 1.0 - jnp.abs(offsets - displace)).astype(jnp.bfloat16)
        product = weight.astype(jnp.float32) * samples
        if displace == 1:
            product = jnp.where(lane == 0, 0.0, pltpu.roll(product, 1, 1))
        elif displace == -1:
            product = jnp.where(lane == LANES - 1, 0.0, pltpu.roll(product, LANES - 1, 1))
        result = product if result is None else result + product
    return result


def sort_blocks(cfg, values, shifts, sensor, window, owner, count, parcel, payload, bases, tops, notes, send):
    owners, cols, rows, room = cfg
    ratio = owners // cols
    planes = owners // ratio
    groups = sensor.shape[0]
    shares = ratio * rows // WIDTH
    bins = planes * WINDOWS * shares
    every = ratio * bins
    third = room // LANES
    lane = lax.broadcasted_iota(jnp.int32, (1, LANES), 1).astype(jnp.float32)
    down = lax.broadcasted_iota(jnp.int32, (LANES, LANES), 0).astype(jnp.float32)
    index = (
        lax.broadcasted_iota(jnp.int32, (groups, LANES), 0) * LANES
        + lax.broadcasted_iota(jnp.int32, (groups, LANES), 1)
    )
    live = index < count[...]
    who = owner[...].astype(jnp.float32)
    what = sensor[...].astype(jnp.float32)
    where = cut(who, ratio)
    share = cut(what, WIDTH)
    number = (where * WINDOWS + window[...].astype(jnp.float32)) * shares + share
    number = jnp.where(live, (who - ratio * where) * bins + number, -1.0)
    local = what - WIDTH * share
    local_top = cut(local, LANES)
    local_low = local - LANES * local_top
    bin_row = lax.broadcasted_iota(jnp.int32, (every, LANES), 0).astype(jnp.float32)
    hot = [jnp.where(number[r:r + 1] == bin_row, 1.0, 0.0) for r in range(groups)]
    before = jnp.concatenate([jnp.where(down < lane, 1.0, 0.0), jnp.ones((LANES, LANES), jnp.float32)], axis=1)
    earlier = jnp.dot(
        jnp.concatenate(hot, axis=0).astype(jnp.bfloat16), before.astype(jnp.bfloat16),
        preferred_element_type=jnp.float32,
    )
    run = jnp.zeros((every, LANES), jnp.float32)
    offset = []
    for r in range(groups):
        part = earlier[r * every:(r + 1) * every]
        offset.append(run + part[:, :LANES])
        run = run + part[:, LANES:]
    upto = run
    shift = 1
    while shift < every:
        upto = upto + jnp.where(bin_row >= shift, pltpu.roll(upto, shift, 0), 0.0)
        shift *= 2
    begin = upto - run
    begin = jnp.concatenate(
        [begin[p * bins:(p + 1) * bins] - begin[p * bins:p * bins + 1] for p in range(ratio)], axis=0
    )
    end = begin + run
    lot_of = cut(bin_row, bins)
    first = begin + lot_of * room
    for r in range(groups):
        spot = jnp.sum(hot[r] * (first + offset[r]), axis=0, keepdims=True)
        spot = jnp.where(live[r:r + 1], spot, -1.0)
        top = cut(jnp.maximum(spot, 0.0), LANES)
        tops[r:r + 1, :] = jnp.where(spot < 0.0, -1.0, top)
        bases[:, r * LANES:(r + 1) * LANES] = jnp.where(spot - top * LANES == down, 1.0, 0.0).astype(jnp.bfloat16)
        at = pl.ds(r * LANES, LANES)
        payload[at, :LANES] = spread_rows(values[at, :], shifts[at, :]).astype(jnp.bfloat16)
        tag = jnp.where(
            down < LANES // 2,
            jnp.broadcast_to(local_top[r:r + 1], (LANES, LANES)),
            jnp.broadcast_to(local_low[r:r + 1], (LANES, LANES)),
        )
        payload[at, LANES:] = jnp.transpose(tag).astype(jnp.bfloat16)
    edge = []
    for column in (begin, end):
        if every < LANES:
            column = jnp.concatenate([column, jnp.zeros((LANES - every, LANES), jnp.float32)], axis=0)
        row = jnp.transpose(column)[0:1]
        high = cut(row, 64)
        edge += [high, row - 64 * high]
    notes[...] = jnp.zeros_like(notes)
    for p in range(ratio):
        for k, row in enumerate(edge):
            notes[p, 2 * third + k:2 * third + k + 1, :] = row
    tile = 4 * LANES
    for p in range(ratio):

        def one_tile(step, carry, p=p):
            strips = []
            for k in range(tile // LANES):
                wanted = (step * (tile // LANES) + k + p * third).astype(jnp.float32)
                chosen = jnp.where(tops[...] == wanted, 1.0, 0.0).astype(jnp.bfloat16)
                strips.append(
                    jnp.concatenate(
                        [bases[:, r * LANES:(r + 1) * LANES] * chosen[r:r + 1] for r in range(groups)], axis=1
                    )
                )
            placed = jnp.dot(jnp.concatenate(strips, axis=0), payload[...], preferred_element_type=jnp.float32)
            parcel[p, pl.ds(pl.multiple_of(step * tile, tile), tile), :] = placed[:, :LANES].astype(jnp.bfloat16)
            for k in range(tile // LANES):
                flat = jnp.transpose(placed[k * LANES:(k + 1) * LANES, LANES:])
                at = step * (tile // LANES) + k
                notes[p, pl.ds(at, 1), :] = flat[0:1]
                notes[p, pl.ds(third + at, 1), :] = flat[LANES // 2:LANES // 2 + 1]
            return carry

        lax.fori_loop(0, room // tile, one_tile, 0)
        parcel[p, room:room + META, :] = notes[p].astype(jnp.bfloat16)
        send(p)


def greet(peers):
    barrier = pltpu.get_barrier_semaphore()
    for peer in peers:
        pl.semaphore_signal(barrier, inc=1, device_id=peer, device_id_type=MESH)
    pl.semaphore_wait(barrier, len(peers))


def deliver_kernel(
    cfg, values_in, shifts_in, sensor_in, window_in, owner_in, count, calib, held, early, part,
    bridge, bridge_sems, values, shifts, sensor, window, owner, load_sems, parcel, relay, payload, bases, tops, notes, send_sems, recv_sems, relay_send, relay_recv, turn_sems,
    side_sems, pass_sems, own_sems, far_send, far_recv,
):
    owners, cols, rows, room = cfg
    ratio = owners // cols
    planes = owners // ratio
    chips = cols // 2
    t, c = lax.axis_index("tm"), lax.axis_index("col")
    core, chip = lax.rem(c, 2), c // 2
    plane, lot = t // ratio, lax.rem(t, ratio)
    first = core == lax.rem(plane, 2)

    def line_of(source, column):
        return lax.rem(source // ratio + lax.rem(source, ratio) + column, chips)

    line = line_of(t, c)
    quarter = rows // 4

    def far_copy(step, turn):
        place = pl.ds(turn * quarter, quarter if turn == 0 else rows - quarter)
        return pltpu.make_async_remote_copy(
            src_ref=calib.at[place, pl.ds(0, PIECE)],
            dst_ref=early.at[step - 1, place],
            send_sem=far_send.at[step - 1, turn],
            recv_sem=far_recv.at[step - 1, turn],
            device_id=(plane * ratio + lax.rem(lot - step + ratio, ratio), c),
            device_id_type=MESH,
        )

    def part_of(k):
        size = (room + META) // PARTS
        return pl.ds(k * size, size)

    def own_copy(origin, source, from_lot, k):
        return pltpu.make_async_copy(
            origin.at[part_of(k)], held.at[source, part_of(k)], own_sems.at[from_lot, k]
        )

    def out_copy(target, k):
        return pltpu.make_async_remote_copy(
            src_ref=parcel.at[target, part_of(k)],
            dst_ref=held.at[t, part_of(k)],
            send_sem=send_sems.at[target, k],
            recv_sem=recv_sems.at[t, k],
            device_id=(c * ratio + target, c),
            device_id_type=MESH,
        )

    def relay_copy(target, k):
        return pltpu.make_async_remote_copy(
            src_ref=parcel.at[target, part_of(k)],
            dst_ref=relay.at[lot, chip, part_of(k)],
            send_sem=relay_send.at[target, k],
            recv_sem=relay_recv.at[lot, chip, k],
            device_id=(plane * ratio + target, line * 2 + core),
            device_id_type=MESH,
        )

    def relay_arrival(from_lot, from_chip, k):
        return pltpu.make_async_remote_copy(
            src_ref=parcel.at[0, part_of(k)],
            dst_ref=relay.at[from_lot, from_chip, part_of(k)],
            send_sem=relay_send.at[0, k],
            recv_sem=relay_recv.at[from_lot, from_chip, k],
            device_id=(plane * ratio + from_lot, from_chip * 2 + core),
            device_id_type=MESH,
        )

    def turn_copy(from_lot, from_chip, k):
        source = plane * ratio + from_lot
        return pltpu.make_async_remote_copy(
            src_ref=relay.at[from_lot, from_chip, part_of(k)],
            dst_ref=held.at[source, part_of(k)],
            send_sem=turn_sems.at[from_lot, from_chip, k],
            recv_sem=recv_sems.at[source, k],
            device_id=((from_chip * 2 + core) * ratio + lot, c),
            device_id_type=MESH,
        )

    def pass_copy(source, k):
        return pltpu.make_async_remote_copy(
            src_ref=held.at[source, part_of(k)],
            dst_ref=held.at[source, part_of(k)],
            send_sem=pass_sems.at[source, k],
            recv_sem=recv_sems.at[source, k],
            device_id=(t, c + 1 - 2 * core),
            device_id_type=MESH,
        )

    def side_copy(source, step, k):
        return pltpu.make_async_remote_copy(
            src_ref=held.at[source, part_of(k)],
            dst_ref=held.at[source, part_of(k)],
            send_sem=side_sems.at[step - 1, source, k],
            recv_sem=recv_sems.at[source, k],
            device_id=(t, lax.rem(chip + step, chips) * 2 + core),
            device_id_type=MESH,
        )

    loads = [
        pltpu.make_async_copy(source, target, load_sems.at[k])
        for k, (source, target) in enumerate(
            ((owner_in, owner), (sensor_in, sensor), (window_in, window), (values_in, values), (shifts_in, shifts))
        )
    ]
    for load in loads:
        load.start()
    bridge_in = pltpu.make_async_copy(
        calib.at[pl.ds(rows - part.shape[0], part.shape[0]), pl.ds(PIECE, PIECE)], bridge, bridge_sems.at[0]
    )
    bridge_out = pltpu.make_async_copy(bridge, part, bridge_sems.at[1])
    bridge_in.start()
    greet(
        [(lax.rem(t + step, owners), c) for step in range(1, owners)]
        + [
            (plane * ratio + lax.rem(lot + side, ratio), lax.rem(c + step, cols))
            for side in range(ratio)
            for step in range(1, cols)
        ]
    )
    for step in range(1, ratio):
        far_copy(step, 0).start()
    for load in loads:
        load.wait()

    def send(target):
        straight = (line == chip) & (target == lot)

        @pl.when(jnp.logical_not(straight))
        def _():
            for k in range(PARTS):
                relay_copy(target, k).start()

        @pl.when(straight & (plane == c))
        def _():
            for k in range(PARTS):
                own_copy(parcel.at[target], t, lot, k).start()

        @pl.when(straight & (plane != c))
        def _():
            for k in range(PARTS):
                out_copy(target, k).start()

    sort_blocks(
        cfg, values, shifts, sensor, window, owner, count, parcel, payload, bases, tops, notes, send
    )

    bridge_in.wait()
    bridge_out.start()

    for step in range(1, ratio):
        far_copy(step, 1).start()

    def each_turn(act):
        for k in range(PARTS):
            for side in range(ratio):
                for step in range(chips):
                    if side or step:
                        from_lot, from_chip = lax.rem(lot + side, ratio), lax.rem(chip + step, chips)
                        column = from_chip * 2 + core

                        @pl.when(line_of(plane * ratio + from_lot, column) == chip)
                        def _():
                            act(from_lot, from_chip, k, column == plane)

    def forward(from_lot, from_chip, k, here):
        relay_arrival(from_lot, from_chip, k).wait_recv()

        @pl.when(here)
        def _():
            own_copy(relay.at[from_lot, from_chip], plane * ratio + from_lot, from_lot, k).start()

        @pl.when(jnp.logical_not(here))
        def _():
            turn_copy(from_lot, from_chip, k).start()

    each_turn(forward)
    table = near_first(planes)
    nearest = [
        (pick(table, plane, turn) * ratio + lax.rem(lot + step, ratio), k)
        for turn in range(planes)
        for step in range(ratio)
        for k in range(PARTS)
    ]

    for source, k in nearest:
        entry = first & (line_of(source, plane) == chip)

        @pl.when(entry & (source // ratio == plane))
        def _():
            own_copy(parcel.at[0], source, lax.rem(source, ratio), k).wait()

        @pl.when(entry & (source // ratio != plane))
        def _():
            pass_copy(source, k).wait_recv()

        @pl.when(entry)
        def _():
            for step in range(1, chips):
                side_copy(source, step, k).start()
            pass_copy(source, k).start()

    for source, k in nearest:

        @pl.when(first & (line_of(source, plane) != chip))
        def _():
            pass_copy(source, k).wait_recv()
            pass_copy(source, k).start()

    for target in range(ratio):
        straight = (line == chip) & (target == lot)

        @pl.when(straight & (plane != c))
        def _():
            for k in range(PARTS):
                out_copy(target, k).wait_send()

        @pl.when(jnp.logical_not(straight))
        def _():
            for k in range(PARTS):
                relay_copy(target, k).wait_send()

    def settle(from_lot, from_chip, k, here):
        @pl.when(jnp.logical_not(here))
        def _():
            turn_copy(from_lot, from_chip, k).wait_send()

    each_turn(settle)

    for source in range(owners):
        for k in range(PARTS):

            @pl.when(first & (line_of(source, plane) == chip))
            def _():
                for step in range(1, chips):
                    side_copy(source, step, k).wait_send()

            @pl.when(first)
            def _():
                pass_copy(source, k).wait_send()

            @pl.when(jnp.logical_not(first))
            def _():
                pass_copy(source, k).wait_recv()

    for step in range(1, ratio):
        for turn in range(2):
            far_copy(step, turn).wait()
    bridge_out.wait()


def deliver(values, shifts, sensor, window, owner, count, calib, owners, cols, capacity):
    ratio = owners // cols
    blocks, length = values.shape
    rows = calib.shape[0]
    room = owners // ratio * capacity
    every = owners * WINDOWS * ratio
    chips = cols // 2
    cfg = (owners, cols, rows, room)
    groups = blocks // LANES
    return pl.pallas_call(
        functools.partial(deliver_kernel, cfg),
        out_shape=[
            jax.ShapeDtypeStruct((owners, room + META, length), jnp.bfloat16),
            jax.ShapeDtypeStruct((ratio - 1, rows, PIECE), jnp.bfloat16),
            jax.ShapeDtypeStruct((rows * 5 // 8, PIECE), jnp.bfloat16),
        ],
        in_specs=[ANY] * 5 + [VMEM, ANY],
        out_specs=[ANY] * 3,
        scratch_shapes=[
            pltpu.VMEM((rows * 5 // 8, PIECE), jnp.bfloat16),
            pltpu.SemaphoreType.DMA((2,)),
            pltpu.VMEM((blocks, length), jnp.bfloat16),
            pltpu.VMEM((blocks, length), jnp.bfloat16),
            pltpu.VMEM((groups, LANES), jnp.int32),
            pltpu.VMEM((groups, LANES), jnp.int32),
            pltpu.VMEM((groups, LANES), jnp.int32),
            pltpu.SemaphoreType.DMA((5,)),
            pltpu.VMEM((ratio, room + META, length), jnp.bfloat16),
            pltpu.VMEM((ratio, chips, room + META, length), jnp.bfloat16),
            pltpu.VMEM((blocks, 2 * LANES), jnp.bfloat16),
            pltpu.VMEM((LANES, blocks), jnp.bfloat16),
            pltpu.VMEM((groups, LANES), jnp.float32),
            pltpu.VMEM((ratio, META, LANES), jnp.float32),
            pltpu.SemaphoreType.DMA((ratio, PARTS)),
            pltpu.SemaphoreType.DMA((owners, PARTS)),
            pltpu.SemaphoreType.DMA((ratio, PARTS)),
            pltpu.SemaphoreType.DMA((ratio, chips, PARTS)),
            pltpu.SemaphoreType.DMA((ratio, chips, PARTS)),
            pltpu.SemaphoreType.DMA((max(chips - 1, 1), owners, PARTS)),
            pltpu.SemaphoreType.DMA((owners, PARTS)),
            pltpu.SemaphoreType.DMA((ratio, PARTS)),
            pltpu.SemaphoreType.DMA((ratio - 1, 2)),
            pltpu.SemaphoreType.DMA((ratio - 1, 2)),
        ],
        compiler_params=pltpu.CompilerParams(
            collective_id=0, has_side_effects=True, vmem_limit_bytes=GRANT
        ),
        cost_estimate=pl.CostEstimate(flops=10 * 10**9, bytes_accessed=10**7, transcendentals=0),
        name="deliver",
    )(values, shifts, sensor, window, owner, count, calib)


def align_kernel(
    cfg, held, aligned, raw, limit, limit_s, contrib, names, stage_a, tags_a, stage_b, tags_b,
    stage, tags, total, ready, sems, out_sems,
):
    sources, room, rows, ratio, planes = cfg
    shares = ratio * rows // WIDTH
    windows = planes * WINDOWS
    bins = windows * shares
    lot = lax.rem(lax.axis_index("tm"), ratio)
    height = room + META
    third = room // LANES
    loads = [
        pltpu.make_async_copy(held.at[s], raw.at[pl.ds(s * height, height)], sems.at[s])
        for s in range(sources)
    ]
    for load in loads:
        load.start()
    for ref in (stage_a, tags_a, stage_b, tags_b):
        ref[...] = jnp.zeros_like(ref)
    tail = pl.ds(sources * room, contrib.shape[0] - sources * room)
    contrib[tail, :] = jnp.zeros_like(contrib[tail, :])
    names[tail, :] = jnp.zeros_like(names[tail, :])
    for s in range(sources):
        loads[s].wait()
        meta = raw[pl.ds(s * height + room, META), :].astype(jnp.float32)
        for side in range(2):
            at = 2 * third + 2 * side
            limit[pl.ds(side * sources + s, 1), :] = (
                meta[at:at + 1] * 64.0 + meta[at + 1:at + 2]
            ).astype(jnp.int32)
        for r in range(third):
            tag = meta[r:r + 1] * float(LANES) + meta[third + r:third + r + 1]
            at = pl.ds(s * room + r * LANES, LANES)
            names[at, :] = jnp.transpose(jnp.broadcast_to(tag, (LANES, LANES)))
            contrib[at, :] = raw[pl.ds(s * height + r * LANES, LANES), :].astype(jnp.float32)
    fetch = pltpu.make_async_copy(limit, limit_s, sems.at[sources])
    fetch.start()
    fetch.wait()

    def put(pair, slot, which, half):
        window = pair * 2 + which
        return pltpu.make_async_copy(
            ready.at[slot, which, half],
            aligned.at[
                window // WINDOWS,
                lax.rem(half - lot + ratio, ratio),
                pl.ds(pl.multiple_of(lax.rem(window, WINDOWS) * LANES, LANES), LANES),
            ],
            out_sems.at[slot, which, half],
        )

    def span_of(window, share, s):
        number = lot * bins + window * shares + share
        begin = limit_s[s, number]
        return s * room + begin, limit_s[sources + s, number] - begin

    def merge(pair, to_stage, to_tags):
        counts, odd = [], []
        for which in range(2):
            longest, largest = 0, 0
            for share in range(shares):
                count = 0
                for s in range(sources):
                    source, extent = span_of(pair * 2 + which, share, s)
                    target = pl.ds(0 if s == 0 else jnp.minimum(count, DEPTH), STEP)
                    to_stage[which * shares + share, target, :] = contrib[pl.ds(source, STEP), :]
                    to_tags[which * shares + share, target, :] = names[pl.ds(source, STEP), :]
                    count = count + extent
                    longest = jnp.maximum(longest, extent)
                counts.append(count)
                largest = jnp.maximum(largest, count)
            odd.append(jnp.where((longest > STEP) | (largest > DEPTH), 1, 0))
        return tuple(counts) + tuple(odd)

    def product(part, tag, first, count, write):
        left = jnp.transpose(part).astype(jnp.bfloat16)
        top = jnp.floor(tag * (1.0 / LANES))
        low = tag - top * LANES
        lane = lax.broadcasted_iota(jnp.int32, (DEPTH, LANES), 1).astype(jnp.float32)
        row = lax.broadcasted_iota(jnp.int32, (DEPTH, LANES), 0)
        base = jnp.where((low == lane) & (row + first < count), 1.0, 0.0).astype(jnp.bfloat16)
        top = top.astype(jnp.bfloat16)
        nothing = jnp.zeros_like(base)
        wide = 4 * LANES
        for n in range(WIDTH // wide):
            hot = jnp.concatenate(
                [
                    jnp.where(top == jnp.bfloat16(n * (wide // LANES) + k), base, nothing)
                    for k in range(wide // LANES)
                ],
                axis=1,
            )
            write(n * wide, wide, jnp.dot(left, hot, preferred_element_type=jnp.float32))

    def spot(slot, which, share, start, size):
        place = share * WIDTH
        return slot, which, place // rows, slice(None), pl.ds(place % rows + start, size)

    def slow(pair, slot, which):
        for share in range(shares):
            count = 0
            stage[...] = jnp.zeros_like(stage)
            for s in range(sources):
                source, extent = span_of(pair * 2 + which, share, s)

                def more(step, inner, source=source, count=count):
                    target = pl.ds(count + step * STEP, STEP)
                    stage[target, :] = contrib[pl.ds(source + step * STEP, STEP), :]
                    tags[target, :] = names[pl.ds(source + step * STEP, STEP), :]
                    return inner

                lax.fori_loop(0, (extent + STEP - 1) // STEP, more, 0)
                count = count + extent
            total[...] = jnp.zeros_like(total)

            def add(start, extent, value):
                total[:, pl.ds(start, extent)] += value

            def chunk(at, inner, count=count):
                place = pl.ds(pl.multiple_of(at * DEPTH, DEPTH), DEPTH)
                product(stage[place, :], tags[place, :], at * DEPTH, count, add)
                return inner

            lax.fori_loop(0, (count + DEPTH - 1) // DEPTH, chunk, 0)
            ready[spot(slot, which, share, 0, WIDTH)] = total[...].astype(jnp.bfloat16)

    def one_pair(pair, slot, found, here, there):
        @pl.when(pair >= 2)
        def _():
            for which in range(2):
                for half in range(ratio):
                    put(pair - 2, slot, which, half).wait()

        later = merge(jnp.minimum(pair + 1, windows // 2 - 1), *there)
        for which in range(2):
            for share in range(shares):
                at = which * shares + share

                def store(start, extent, value, which=which, share=share):
                    ready[spot(slot, which, share, start, extent)] = value.astype(jnp.bfloat16)

                product(here[0][at, pl.ds(0, DEPTH), :], here[1][at, pl.ds(0, DEPTH), :], 0, found[at], store)
        for which in range(2):

            @pl.when(found[2 * shares + which] > 0)
            def _():
                slow(pair, slot, which)

            for half in range(ratio):
                put(pair, slot, which, half).start()
        return later

    a, b = (stage_a, tags_a), (stage_b, tags_b)

    def two_pairs(step, found):
        found = one_pair(step * 2, 0, found, a, b)
        return one_pair(step * 2 + 1, 1, found, b, a)

    lax.fori_loop(0, windows // 4, two_pairs, merge(jnp.int32(0), *a))
    for slot in range(2):
        for which in range(2):
            for half in range(ratio):
                put(jnp.int32(windows // 2 - 2 + slot), slot, which, half).wait()


def align(held, rows, ratio, planes, capacity):
    sources, height, length = held.shape
    room = height - META
    deep = -(-(sources * capacity + STEP) // DEPTH) * DEPTH
    shares = ratio * rows // WIDTH
    cfg = (sources, room, rows, ratio, planes)
    short = pltpu.VMEM((2 * shares, DEPTH + STEP, LANES), jnp.float32)
    return pl.pallas_call(
        functools.partial(align_kernel, cfg),
        out_shape=jax.ShapeDtypeStruct((planes, ratio, WINDOWS * length, rows), jnp.bfloat16),
        in_specs=[ANY],
        out_specs=ANY,
        scratch_shapes=[
            pltpu.VMEM((sources * height, length), jnp.bfloat16),
            pltpu.VMEM((2 * sources, LANES), jnp.int32),
            pltpu.SMEM((2 * sources, LANES), jnp.int32),
            pltpu.VMEM((sources * room + STEP, length), jnp.float32),
            pltpu.VMEM((sources * room + STEP, LANES), jnp.float32),
            short,
            short,
            short,
            short,
            pltpu.VMEM((deep, length), jnp.float32),
            pltpu.VMEM((deep, LANES), jnp.float32),
            pltpu.VMEM((length, WIDTH), jnp.float32),
            pltpu.VMEM((2, 2, ratio, length, rows), jnp.bfloat16),
            pltpu.SemaphoreType.DMA((sources + 1,)),
            pltpu.SemaphoreType.DMA((2, 2, ratio)),
        ],
        compiler_params=pltpu.CompilerParams(vmem_limit_bytes=GRANT),
        cost_estimate=pl.CostEstimate(flops=10 * 10**9, bytes_accessed=2 * 10**7, transcendentals=0),
        name="align",
    )(held)


def far_first(planes):
    return [sorted(range(planes), key=lambda p: (-abs(p - z), -p)) for z in range(planes)]


def reduce_kernel(
    cfg, aligned, calib, early, later, out, left, near, far, stage, up, down, kept, total, answer,
    left_sems, near_sems, early_sems, later_sems, far_send, far_recv, up_send, up_recv, down_send, down_recv, out_sems,
):
    planes, ratio, pieces = cfg
    t, c = lax.axis_index("tm"), lax.axis_index("col")
    plane, lot = t // ratio, lax.rem(t, ratio)
    rows = calib.shape[0]
    gap = rows - later.shape[1]
    split = rows // 2
    order = far_first(planes)

    def columns(piece):
        return pl.ds(pl.multiple_of(piece * PIECE, PIECE), PIECE)

    def far_copy(step, piece, part):
        place = pl.ds(0, gap) if part == 2 else pl.ds(part * split, split)
        return pltpu.make_async_remote_copy(
            src_ref=calib.at[place, columns(piece)],
            dst_ref=far.at[step - 1, piece, place],
            send_sem=far_send.at[step - 1, piece, part],
            recv_sem=far_recv.at[step - 1, piece, part],
            device_id=(plane * ratio + lax.rem(lot - step + ratio, ratio), c),
            device_id_type=MESH,
        )

    def target(turn):
        return pick(order, plane, turn)

    def near_load(piece):
        return pltpu.make_async_copy(calib.at[:, columns(piece)], near.at[piece], near_sems.at[piece])

    def early_load(step):
        return pltpu.make_async_copy(
            early.at[step - 1], far.at[step - 1, 0], early_sems.at[step - 1]
        )

    def later_load(step):
        return pltpu.make_async_copy(
            later.at[step - 1], far.at[step - 1, 1, pl.ds(gap, rows - gap)], later_sems.at[step - 1]
        )

    def left_load(turn):
        where = target(turn)
        return pltpu.make_async_copy(aligned.at[where], left.at[where], left_sems.at[turn])

    steps = range(1, ratio)
    opening = [left_load(0), near_load(0)] + [early_load(step) for step in steps]
    for load in opening:
        load.start()
    barrier = pltpu.get_barrier_semaphore()
    peers = [(True, (plane * ratio + lax.rem(lot + step, ratio), c)) for step in steps]
    peers += [(plane > 0, (t - ratio, c)), (plane < planes - 1, (t + ratio, c))]
    for near_by, peer in peers:

        @pl.when(near_by)
        def _():
            pl.semaphore_signal(barrier, inc=1, device_id=peer, device_id_type=MESH)

    pl.semaphore_wait(
        barrier, ratio - 1 + jnp.where(plane > 0, 1, 0) + jnp.where(plane < planes - 1, 1, 0)
    )

    late = [(1, 2)] + [(piece, part) for piece in range(2, pieces) for part in range(2)]
    for piece, part in late:
        for step in steps:
            far_copy(step, piece, part).start()
    for load in opening:
        load.wait()
    for turn in range(1, planes):
        left_load(turn).start()
    for piece in range(1, pieces):
        near_load(piece).start()
    for step in steps:
        later_load(step).start()

    def hop(piece, where, buffer, sends, recvs, side):
        return pltpu.make_async_remote_copy(
            src_ref=stage.at[piece, where],
            dst_ref=buffer.at[piece, where],
            send_sem=sends.at[piece, where],
            recv_sem=recvs.at[piece, where],
            device_id=(t + side * ratio, c),
            device_id_type=MESH,
        )

    def go_up(piece, where):
        return hop(piece, where, up, up_send, up_recv, 1)

    def go_down(piece, where):
        return hop(piece, where, down, down_send, down_recv, -1)

    def one_piece(piece, carry):
        @pl.when(piece > 0)
        def _():
            near_load(piece).wait()

        @pl.when(piece == 1)
        def _():
            for step in steps:
                later_load(step).wait()
                far_copy(step, 1, 2).wait_recv()

        @pl.when(piece > 1)
        def _():
            for step in steps:
                for part in range(2):
                    far_copy(step, piece, part).wait_recv()

        def one_turn(turn, inner):
            where = target(turn)

            @pl.when((piece == 0) & (turn > 0))
            def _():
                left_load(turn).wait()

            value = jnp.dot(left[where, 0], near[piece], preferred_element_type=jnp.float32)
            for step in range(1, ratio):
                value = value + jnp.dot(
                    left[where, step], far[step - 1, piece], preferred_element_type=jnp.float32
                )
            total[...] = value

            @pl.when((where > plane) & (plane > 0))
            def _():
                go_up(piece, where).wait_recv()
                stage[piece, where] = (total[...] + up[piece, where].astype(jnp.float32)).astype(jnp.bfloat16)

            @pl.when((where < plane) & (plane < planes - 1))
            def _():
                go_down(piece, where).wait_recv()
                stage[piece, where] = (total[...] + down[piece, where].astype(jnp.float32)).astype(jnp.bfloat16)

            @pl.when(((where > plane) & (plane == 0)) | ((where < plane) & (plane == planes - 1)))
            def _():
                stage[piece, where] = total[...].astype(jnp.bfloat16)

            @pl.when(where > plane)
            def _():
                go_up(piece, where).start()

            @pl.when(where < plane)
            def _():
                go_down(piece, where).start()

            @pl.when(where == plane)
            def _():
                kept[piece] = total[...]

            return inner

        lax.fori_loop(0, planes, one_turn, 0)
        return carry

    lax.fori_loop(0, pieces, one_piece, 0)

    def put(piece):
        return pltpu.make_async_copy(
            answer.at[piece],
            out.at[:, pl.ds(pl.multiple_of(piece * PIECE, PIECE), PIECE)],
            out_sems.at[piece],
        )

    def finish(piece, carry):
        @pl.when(plane > 0)
        def _():
            go_up(piece, plane).wait_recv()
            kept[piece] += up[piece, plane].astype(jnp.float32)

        @pl.when(plane < planes - 1)
        def _():
            go_down(piece, plane).wait_recv()
            kept[piece] += down[piece, plane].astype(jnp.float32)

        answer[piece] = kept[piece].astype(jnp.bfloat16)
        put(piece).start()
        return carry

    lax.fori_loop(0, pieces, finish, 0)

    def drain(piece, carry):
        put(piece).wait()
        for where in range(planes):
            @pl.when(where > plane)
            def _():
                go_up(piece, where).wait_send()

            @pl.when(where < plane)
            def _():
                go_down(piece, where).wait_send()

        return carry

    lax.fori_loop(0, pieces, drain, 0)
    for piece, part in late:
        for step in steps:
            far_copy(step, piece, part).wait_send()


def reduce(aligned, calib, early, later):
    planes, ratio, height, rows = aligned.shape
    outputs = calib.shape[1]
    pieces = outputs // PIECE
    cfg = (planes, ratio, pieces)
    far = (ratio - 1, pieces, 3)
    hops = (pieces, planes)
    return pl.pallas_call(
        functools.partial(reduce_kernel, cfg),
        out_shape=jax.ShapeDtypeStruct((height, outputs), jnp.bfloat16),
        in_specs=[ANY] * 4,
        out_specs=ANY,
        scratch_shapes=[
            pltpu.VMEM((planes, ratio, height, rows), jnp.bfloat16),
            pltpu.VMEM((pieces, rows, PIECE), jnp.bfloat16),
            pltpu.VMEM((ratio - 1, pieces, rows, PIECE), jnp.bfloat16),
            pltpu.VMEM((pieces, planes, height, PIECE), jnp.bfloat16),
            pltpu.VMEM((pieces, planes, height, PIECE), jnp.bfloat16),
            pltpu.VMEM((pieces, planes, height, PIECE), jnp.bfloat16),
            pltpu.VMEM((pieces, height, PIECE), jnp.float32),
            pltpu.VMEM((height, PIECE), jnp.float32),
            pltpu.VMEM((pieces, height, PIECE), jnp.bfloat16),
            pltpu.SemaphoreType.DMA((planes,)),
            pltpu.SemaphoreType.DMA((pieces,)),
            pltpu.SemaphoreType.DMA((ratio - 1,)),
            pltpu.SemaphoreType.DMA((ratio - 1,)),
            pltpu.SemaphoreType.DMA(far),
            pltpu.SemaphoreType.DMA(far),
            pltpu.SemaphoreType.DMA(hops),
            pltpu.SemaphoreType.DMA(hops),
            pltpu.SemaphoreType.DMA(hops),
            pltpu.SemaphoreType.DMA(hops),
            pltpu.SemaphoreType.DMA((pieces,)),
        ],
        compiler_params=pltpu.CompilerParams(
            collective_id=1, has_side_effects=True, vmem_limit_bytes=GRANT
        ),
        cost_estimate=pl.CostEstimate(flops=20 * 10**9, bytes_accessed=3 * 10**7, transcendentals=0),
        name="reduce",
    )(aligned, calib, early, later)


def per_device(
    block_values, block_shifts, block_sensor, block_window, block_owner, block_counts, calibration
):
    owners = lax.axis_size("tm")
    cols = lax.axis_size("col")
    ratio = owners // cols
    planes = owners // ratio
    rows, outputs = calibration.shape
    blocks = block_values.shape[1]
    capacity = min(blocks, blocks * 3 // (2 * owners))
    def shifted(step):
        return [((t // ratio) * ratio + (t % ratio + step) % ratio, t) for t in range(owners)]

    by_lane = (blocks // LANES, LANES)
    held, early, part = deliver(
        block_values[0], block_shifts[0], block_sensor.reshape(by_lane), block_window.reshape(by_lane),
        block_owner.reshape(by_lane), block_counts, calibration, owners, cols, capacity,
    )
    later = jnp.stack([lax.ppermute(part, "tm", shifted(step)) for step in range(1, ratio)])
    aligned = align(held, rows, ratio, planes, capacity)
    return reduce(aligned, calibration, early, later)


def solution(mesh):
    placed = (
        P("col", "tm", None),
        P("col", "tm", None),
        P("col", "tm"),
        P("col", "tm"),
        P("col", "tm", None),
        P("col", "tm"),
        P("tm", "col"),
    )
    return jax.shard_map(
        per_device, mesh=mesh, in_specs=placed, out_specs=P("tm", "col"), check_vma=False
    )
```

```python
import functools

import jax
import jax.numpy as jnp
from jax import lax
from jax.experimental import pallas as pl
from jax.experimental.pallas import tpu as pltpu
from jax.sharding import PartitionSpec as P

WINDOWS = 4
LANES = 128
META = 64
DEPTH = 256
STEP = 48
WIDTH = 1024
PARTS = 4
STRIPS = 2
PIECE = 256
GRANT = 67_000_000


ANY = pl.BlockSpec(memory_space=pl.ANY)
VMEM = pl.BlockSpec(memory_space=pltpu.VMEM)
MESH = pl.DeviceIdType.MESH


def cut(whole, size):
    return jnp.floor((whole + 0.5) * (1.0 / size))


def near_first(groups):
    return [sorted(range(groups), key=lambda g: (abs(g - me), g)) for me in range(groups)]


def pick(table, mine, turn):
    chosen = jnp.int32(0)
    for own, row in enumerate(table):
        value = jnp.int32(0)
        for at, entry in enumerate(row):
            value = value + jnp.where(turn == at, entry, 0)
        chosen = chosen + jnp.where(mine == own, value, 0)
    return chosen


def spread_rows(values, shifts):
    samples = values.astype(jnp.float32)
    offsets = shifts.astype(jnp.float32)
    lane = lax.broadcasted_iota(jnp.int32, samples.shape, 1)
    result = None
    for displace in (-1, 0, 1):
        weight = jnp.maximum(0.0, 1.0 - jnp.abs(offsets - displace)).astype(jnp.bfloat16)
        product = weight.astype(jnp.float32) * samples
        if displace == 1:
            product = jnp.where(lane == 0, 0.0, pltpu.roll(product, 1, 1))
        elif displace == -1:
            product = jnp.where(lane == LANES - 1, 0.0, pltpu.roll(product, LANES - 1, 1))
        result = product if result is None else result + product
    return result


def sort_blocks(cfg, values, shifts, sensor, window, owner, count, parcel, payload, bases, tops, notes, send):
    owners, cols, rows, room = cfg
    ratio = owners // cols
    planes = owners // ratio
    groups = sensor.shape[0]
    shares = ratio * rows // WIDTH
    bins = planes * WINDOWS * shares
    every = ratio * bins
    third = room // LANES
    lane = lax.broadcasted_iota(jnp.int32, (1, LANES), 1).astype(jnp.float32)
    down = lax.broadcasted_iota(jnp.int32, (LANES, LANES), 0).astype(jnp.float32)
    index = (
        lax.broadcasted_iota(jnp.int32, (groups, LANES), 0) * LANES
        + lax.broadcasted_iota(jnp.int32, (groups, LANES), 1)
    )
    live = index < count[...]
    who = owner[...].astype(jnp.float32)
    what = sensor[...].astype(jnp.float32)
    where = cut(who, ratio)
    share = cut(what, WIDTH)
    number = (where * WINDOWS + window[...].astype(jnp.float32)) * shares + share
    number = jnp.where(live, (who - ratio * where) * bins + number, -1.0)
    local = what - WIDTH * share
    local_top = cut(local, LANES)
    local_low = local - LANES * local_top
    bin_row = lax.broadcasted_iota(jnp.int32, (every, LANES), 0).astype(jnp.float32)
    hot = [jnp.where(number[r:r + 1] == bin_row, 1.0, 0.0) for r in range(groups)]
    before = jnp.concatenate([jnp.where(down < lane, 1.0, 0.0), jnp.ones((LANES, LANES), jnp.float32)], axis=1)
    earlier = jnp.dot(
        jnp.concatenate(hot, axis=0).astype(jnp.bfloat16), before.astype(jnp.bfloat16),
        preferred_element_type=jnp.float32,
    )
    run = jnp.zeros((every, LANES), jnp.float32)
    offset = []
    for r in range(groups):
        part = earlier[r * every:(r + 1) * every]
        offset.append(run + part[:, :LANES])
        run = run + part[:, LANES:]
    upto = run
    shift = 1
    while shift < every:
        upto = upto + jnp.where(bin_row >= shift, pltpu.roll(upto, shift, 0), 0.0)
        shift *= 2
    begin = upto - run
    begin = jnp.concatenate(
        [begin[p * bins:(p + 1) * bins] - begin[p * bins:p * bins + 1] for p in range(ratio)], axis=0
    )
    end = begin + run
    lot_of = cut(bin_row, bins)
    first = begin + lot_of * room
    for r in range(groups):
        spot = jnp.sum(hot[r] * (first + offset[r]), axis=0, keepdims=True)
        spot = jnp.where(live[r:r + 1], spot, -1.0)
        top = cut(jnp.maximum(spot, 0.0), LANES)
        tops[r:r + 1, :] = jnp.where(spot < 0.0, -1.0, top)
        bases[:, r * LANES:(r + 1) * LANES] = jnp.where(spot - top * LANES == down, 1.0, 0.0).astype(jnp.bfloat16)
        at = pl.ds(r * LANES, LANES)
        payload[at, :LANES] = spread_rows(values[at, :], shifts[at, :]).astype(jnp.bfloat16)
        tag = jnp.where(
            down < LANES // 2,
            jnp.broadcast_to(local_top[r:r + 1], (LANES, LANES)),
            jnp.broadcast_to(local_low[r:r + 1], (LANES, LANES)),
        )
        payload[at, LANES:] = jnp.transpose(tag).astype(jnp.bfloat16)
    edge = []
    for column in (begin, end):
        if every < LANES:
            column = jnp.concatenate([column, jnp.zeros((LANES - every, LANES), jnp.float32)], axis=0)
        row = jnp.transpose(column)[0:1]
        high = cut(row, 64)
        edge += [high, row - 64 * high]
    notes[...] = jnp.zeros_like(notes)
    for p in range(ratio):
        for k, row in enumerate(edge):
            notes[p, 2 * third + k:2 * third + k + 1, :] = row
    tile = 4 * LANES
    for p in range(ratio):

        def one_tile(step, carry, p=p):
            strips = []
            for k in range(tile // LANES):
                wanted = (step * (tile // LANES) + k + p * third).astype(jnp.float32)
                chosen = jnp.where(tops[...] == wanted, 1.0, 0.0).astype(jnp.bfloat16)
                strips.append(
                    jnp.concatenate(
                        [bases[:, r * LANES:(r + 1) * LANES] * chosen[r:r + 1] for r in range(groups)], axis=1
                    )
                )
            placed = jnp.dot(jnp.concatenate(strips, axis=0), payload[...], preferred_element_type=jnp.float32)
            parcel[p, pl.ds(pl.multiple_of(step * tile, tile), tile), :] = placed[:, :LANES].astype(jnp.bfloat16)
            for k in range(tile // LANES):
                flat = jnp.transpose(placed[k * LANES:(k + 1) * LANES, LANES:])
                at = step * (tile // LANES) + k
                notes[p, pl.ds(at, 1), :] = flat[0:1]
                notes[p, pl.ds(third + at, 1), :] = flat[LANES // 2:LANES // 2 + 1]
            return carry

        lax.fori_loop(0, room // tile, one_tile, 0)
        parcel[p, room:room + META, :] = notes[p].astype(jnp.bfloat16)
        send(p)


def greet(peers):
    barrier = pltpu.get_barrier_semaphore()
    for peer in peers:
        pl.semaphore_signal(barrier, inc=1, device_id=peer, device_id_type=MESH)
    pl.semaphore_wait(barrier, len(peers))


def deliver_kernel(
    cfg, values_in, shifts_in, sensor_in, window_in, owner_in, count, calib, held, early, part,
    bridge, bridge_sems, values, shifts, sensor, window, owner, load_sems, parcel, relay, payload, bases, tops, notes, send_sems, recv_sems, relay_send, relay_recv, turn_sems,
    side_sems, pass_sems, own_sems, far_send, far_recv,
):
    owners, cols, rows, room = cfg
    ratio = owners // cols
    planes = owners // ratio
    chips = cols // 2
    t, c = lax.axis_index("tm"), lax.axis_index("col")
    core, chip = lax.rem(c, 2), c // 2
    plane, lot = t // ratio, lax.rem(t, ratio)
    first = core == lax.rem(plane, 2)

    def line_of(source, column):
        return lax.rem(source // ratio + lax.rem(source, ratio) + column, chips)

    line = line_of(t, c)
    quarter = rows // 4

    def far_copy(step, turn):
        place = pl.ds(turn * quarter, quarter if turn == 0 else rows - quarter)
        return pltpu.make_async_remote_copy(
            src_ref=calib.at[place, pl.ds(0, PIECE)],
            dst_ref=early.at[step - 1, place],
            send_sem=far_send.at[step - 1, turn],
            recv_sem=far_recv.at[step - 1, turn],
            device_id=(plane * ratio + lax.rem(lot - step + ratio, ratio), c),
            device_id_type=MESH,
        )

    def part_of(k):
        size = (room + META) // PARTS
        return pl.ds(k * size, size)

    def own_copy(origin, source, from_lot, k):
        return pltpu.make_async_copy(
            origin.at[part_of(k)], held.at[source, part_of(k)], own_sems.at[from_lot, k]
        )

    def out_copy(target, k):
        return pltpu.make_async_remote_copy(
            src_ref=parcel.at[target, part_of(k)],
            dst_ref=held.at[t, part_of(k)],
            send_sem=send_sems.at[target, k],
            recv_sem=recv_sems.at[t, k],
            device_id=(c * ratio + target, c),
            device_id_type=MESH,
        )

    def relay_copy(target, k):
        return pltpu.make_async_remote_copy(
            src_ref=parcel.at[target, part_of(k)],
            dst_ref=relay.at[lot, chip, part_of(k)],
            send_sem=relay_send.at[target, k],
            recv_sem=relay_recv.at[lot, chip, k],
            device_id=(plane * ratio + target, line * 2 + core),
            device_id_type=MESH,
        )

    def relay_arrival(from_lot, from_chip, k):
        return pltpu.make_async_remote_copy(
            src_ref=parcel.at[0, part_of(k)],
            dst_ref=relay.at[from_lot, from_chip, part_of(k)],
            send_sem=relay_send.at[0, k],
            recv_sem=relay_recv.at[from_lot, from_chip, k],
            device_id=(plane * ratio + from_lot, from_chip * 2 + core),
            device_id_type=MESH,
        )

    def turn_copy(from_lot, from_chip, k):
        source = plane * ratio + from_lot
        return pltpu.make_async_remote_copy(
            src_ref=relay.at[from_lot, from_chip, part_of(k)],
            dst_ref=held.at[source, part_of(k)],
            send_sem=turn_sems.at[from_lot, from_chip, k],
            recv_sem=recv_sems.at[source, k],
            device_id=((from_chip * 2 + core) * ratio + lot, c),
            device_id_type=MESH,
        )

    def pass_copy(source, k):
        return pltpu.make_async_remote_copy(
            src_ref=held.at[source, part_of(k)],
            dst_ref=held.at[source, part_of(k)],
            send_sem=pass_sems.at[source, k],
            recv_sem=recv_sems.at[source, k],
            device_id=(t, c + 1 - 2 * core),
            device_id_type=MESH,
        )

    def side_copy(source, step, k):
        return pltpu.make_async_remote_copy(
            src_ref=held.at[source, part_of(k)],
            dst_ref=held.at[source, part_of(k)],
            send_sem=side_sems.at[step - 1, source, k],
            recv_sem=recv_sems.at[source, k],
            device_id=(t, lax.rem(chip + step, chips) * 2 + core),
            device_id_type=MESH,
        )

    loads = [
        pltpu.make_async_copy(source, target, load_sems.at[k])
        for k, (source, target) in enumerate(
            ((owner_in, owner), (sensor_in, sensor), (window_in, window), (values_in, values), (shifts_in, shifts))
        )
    ]
    for load in loads:
        load.start()
    bridge_in = pltpu.make_async_copy(
        calib.at[pl.ds(rows - part.shape[0], part.shape[0]), pl.ds(PIECE, PIECE)], bridge, bridge_sems.at[0]
    )
    bridge_out = pltpu.make_async_copy(bridge, part, bridge_sems.at[1])
    bridge_in.start()
    greet(
        [(lax.rem(t + step, owners), c) for step in range(1, owners)]
        + [
            (plane * ratio + lax.rem(lot + side, ratio), lax.rem(c + step, cols))
            for side in range(ratio)
            for step in range(1, cols)
        ]
    )
    for step in range(1, ratio):
        far_copy(step, 0).start()
    for load in loads:
        load.wait()

    def send(target):
        straight = (line == chip) & (target == lot)

        @pl.when(jnp.logical_not(straight))
        def _():
            for k in range(PARTS):
                relay_copy(target, k).start()

        @pl.when(straight & (plane == c))
        def _():
            for k in range(PARTS):
                own_copy(parcel.at[target], t, lot, k).start()

        @pl.when(straight & (plane != c))
        def _():
            for k in range(PARTS):
                out_copy(target, k).start()

    sort_blocks(
        cfg, values, shifts, sensor, window, owner, count, parcel, payload, bases, tops, notes, send
    )

    bridge_in.wait()
    bridge_out.start()

    for step in range(1, ratio):
        far_copy(step, 1).start()

    def each_turn(act):
        for k in range(PARTS):
            for side in range(ratio):
                for step in range(chips):
                    if side or step:
                        from_lot, from_chip = lax.rem(lot + side, ratio), lax.rem(chip + step, chips)
                        column = from_chip * 2 + core

                        @pl.when(line_of(plane * ratio + from_lot, column) == chip)
                        def _():
                            act(from_lot, from_chip, k, column == plane)

    def forward(from_lot, from_chip, k, here):
        relay_arrival(from_lot, from_chip, k).wait_recv()

        @pl.when(here)
        def _():
            own_copy(relay.at[from_lot, from_chip], plane * ratio + from_lot, from_lot, k).start()

        @pl.when(jnp.logical_not(here))
        def _():
            turn_copy(from_lot, from_chip, k).start()

    each_turn(forward)
    table = near_first(planes)
    nearest = [
        (pick(table, plane, turn) * ratio + lax.rem(lot + step, ratio), k)
        for turn in range(planes)
        for step in range(ratio)
        for k in range(PARTS)
    ]

    for source, k in nearest:
        entry = first & (line_of(source, plane) == chip)

        @pl.when(entry & (source // ratio == plane))
        def _():
            own_copy(parcel.at[0], source, lax.rem(source, ratio), k).wait()

        @pl.when(entry & (source // ratio != plane))
        def _():
            pass_copy(source, k).wait_recv()

        @pl.when(entry)
        def _():
            for step in range(1, chips):
                side_copy(source, step, k).start()
            pass_copy(source, k).start()

    for source, k in nearest:

        @pl.when(first & (line_of(source, plane) != chip))
        def _():
            pass_copy(source, k).wait_recv()
            pass_copy(source, k).start()

    for target in range(ratio):
        straight = (line == chip) & (target == lot)

        @pl.when(straight & (plane != c))
        def _():
            for k in range(PARTS):
                out_copy(target, k).wait_send()

        @pl.when(jnp.logical_not(straight))
        def _():
            for k in range(PARTS):
                relay_copy(target, k).wait_send()

    def settle(from_lot, from_chip, k, here):
        @pl.when(jnp.logical_not(here))
        def _():
            turn_copy(from_lot, from_chip, k).wait_send()

    each_turn(settle)

    for source in range(owners):
        for k in range(PARTS):

            @pl.when(first & (line_of(source, plane) == chip))
            def _():
                for step in range(1, chips):
                    side_copy(source, step, k).wait_send()

            @pl.when(first)
            def _():
                pass_copy(source, k).wait_send()

            @pl.when(jnp.logical_not(first))
            def _():
                pass_copy(source, k).wait_recv()

    for step in range(1, ratio):
        for turn in range(2):
            far_copy(step, turn).wait()
    bridge_out.wait()


def deliver(values, shifts, sensor, window, owner, count, calib, owners, cols, capacity):
    ratio = owners // cols
    blocks, length = values.shape
    rows = calib.shape[0]
    room = owners // ratio * capacity
    every = owners * WINDOWS * ratio
    chips = cols // 2
    cfg = (owners, cols, rows, room)
    groups = blocks // LANES
    return pl.pallas_call(
        functools.partial(deliver_kernel, cfg),
        out_shape=[
            jax.ShapeDtypeStruct((owners, room + META, length), jnp.bfloat16),
            jax.ShapeDtypeStruct((ratio - 1, rows, PIECE), jnp.bfloat16),
            jax.ShapeDtypeStruct((rows * 5 // 8, PIECE), jnp.bfloat16),
        ],
        in_specs=[ANY] * 5 + [VMEM, ANY],
        out_specs=[ANY] * 3,
        scratch_shapes=[
            pltpu.VMEM((rows * 5 // 8, PIECE), jnp.bfloat16),
            pltpu.SemaphoreType.DMA((2,)),
            pltpu.VMEM((blocks, length), jnp.bfloat16),
            pltpu.VMEM((blocks, length), jnp.bfloat16),
            pltpu.VMEM((groups, LANES), jnp.int32),
            pltpu.VMEM((groups, LANES), jnp.int32),
            pltpu.VMEM((groups, LANES), jnp.int32),
            pltpu.SemaphoreType.DMA((5,)),
            pltpu.VMEM((ratio, room + META, length), jnp.bfloat16),
            pltpu.VMEM((ratio, chips, room + META, length), jnp.bfloat16),
            pltpu.VMEM((blocks, 2 * LANES), jnp.bfloat16),
            pltpu.VMEM((LANES, blocks), jnp.bfloat16),
            pltpu.VMEM((groups, LANES), jnp.float32),
            pltpu.VMEM((ratio, META, LANES), jnp.float32),
            pltpu.SemaphoreType.DMA((ratio, PARTS)),
            pltpu.SemaphoreType.DMA((owners, PARTS)),
            pltpu.SemaphoreType.DMA((ratio, PARTS)),
            pltpu.SemaphoreType.DMA((ratio, chips, PARTS)),
            pltpu.SemaphoreType.DMA((ratio, chips, PARTS)),
            pltpu.SemaphoreType.DMA((max(chips - 1, 1), owners, PARTS)),
            pltpu.SemaphoreType.DMA((owners, PARTS)),
            pltpu.SemaphoreType.DMA((ratio, PARTS)),
            pltpu.SemaphoreType.DMA((ratio - 1, 2)),
            pltpu.SemaphoreType.DMA((ratio - 1, 2)),
        ],
        compiler_params=pltpu.CompilerParams(
            collective_id=0, has_side_effects=True, vmem_limit_bytes=GRANT
        ),
        cost_estimate=pl.CostEstimate(flops=10 * 10**9, bytes_accessed=10**7, transcendentals=0),
        name="deliver",
    )(values, shifts, sensor, window, owner, count, calib)


def align_kernel(
    cfg, held, aligned, raw, limit, limit_s, contrib, names, stage_a, tags_a, stage_b, tags_b,
    stage, tags, total, ready, sems, out_sems,
):
    sources, room, rows, ratio, planes = cfg
    shares = ratio * rows // WIDTH
    windows = planes * WINDOWS
    bins = windows * shares
    lot = lax.rem(lax.axis_index("tm"), ratio)
    height = room + META
    third = room // LANES
    loads = [
        pltpu.make_async_copy(held.at[s], raw.at[pl.ds(s * height, height)], sems.at[s])
        for s in range(sources)
    ]
    for load in loads:
        load.start()
    for ref in (stage_a, tags_a, stage_b, tags_b):
        ref[...] = jnp.zeros_like(ref)
    tail = pl.ds(sources * room, contrib.shape[0] - sources * room)
    contrib[tail, :] = jnp.zeros_like(contrib[tail, :])
    names[tail, :] = jnp.zeros_like(names[tail, :])
    for s in range(sources):
        loads[s].wait()
        meta = raw[pl.ds(s * height + room, META), :].astype(jnp.float32)
        for side in range(2):
            at = 2 * third + 2 * side
            limit[pl.ds(side * sources + s, 1), :] = (
                meta[at:at + 1] * 64.0 + meta[at + 1:at + 2]
            ).astype(jnp.int32)
        for r in range(third):
            tag = meta[r:r + 1] * float(LANES) + meta[third + r:third + r + 1]
            at = pl.ds(s * room + r * LANES, LANES)
            names[at, :] = jnp.transpose(jnp.broadcast_to(tag, (LANES, LANES)))
            contrib[at, :] = raw[pl.ds(s * height + r * LANES, LANES), :].astype(jnp.float32)
    fetch = pltpu.make_async_copy(limit, limit_s, sems.at[sources])
    fetch.start()
    fetch.wait()

    def put(pair, slot, which, half):
        window = pair * 2 + which
        return pltpu.make_async_copy(
            ready.at[slot, which, half],
            aligned.at[
                window // WINDOWS,
                lax.rem(half - lot + ratio, ratio),
                pl.ds(pl.multiple_of(lax.rem(window, WINDOWS) * LANES, LANES), LANES),
            ],
            out_sems.at[slot, which, half],
        )

    def span_of(window, share, s):
        number = lot * bins + window * shares + share
        begin = limit_s[s, number]
        return s * room + begin, limit_s[sources + s, number] - begin

    def merge(pair, to_stage, to_tags):
        counts, odd = [], []
        for which in range(2):
            longest, largest = 0, 0
            for share in range(shares):
                count = 0
                for s in range(sources):
                    source, extent = span_of(pair * 2 + which, share, s)
                    target = pl.ds(0 if s == 0 else jnp.minimum(count, DEPTH), STEP)
                    to_stage[which * shares + share, target, :] = contrib[pl.ds(source, STEP), :]
                    to_tags[which * shares + share, target, :] = names[pl.ds(source, STEP), :]
                    count = count + extent
                    longest = jnp.maximum(longest, extent)
                counts.append(count)
                largest = jnp.maximum(largest, count)
            odd.append(jnp.where((longest > STEP) | (largest > DEPTH), 1, 0))
        return tuple(counts) + tuple(odd)

    def product(part, tag, first, count, write):
        left = jnp.transpose(part).astype(jnp.bfloat16)
        top = jnp.floor(tag * (1.0 / LANES))
        low = tag - top * LANES
        lane = lax.broadcasted_iota(jnp.int32, (DEPTH, LANES), 1).astype(jnp.float32)
        row = lax.broadcasted_iota(jnp.int32, (DEPTH, LANES), 0)
        base = jnp.where((low == lane) & (row + first < count), 1.0, 0.0).astype(jnp.bfloat16)
        top = top.astype(jnp.bfloat16)
        nothing = jnp.zeros_like(base)
        wide = 4 * LANES
        for n in range(WIDTH // wide):
            hot = jnp.concatenate(
                [
                    jnp.where(top == jnp.bfloat16(n * (wide // LANES) + k), base, nothing)
                    for k in range(wide // LANES)
                ],
                axis=1,
            )
            write(n * wide, wide, jnp.dot(left, hot, preferred_element_type=jnp.float32))

    def spot(slot, which, share, start, size):
        place = share * WIDTH
        return slot, which, place // rows, slice(None), pl.ds(place % rows + start, size)

    def slow(pair, slot, which):
        for share in range(shares):
            count = 0
            stage[...] = jnp.zeros_like(stage)
            for s in range(sources):
                source, extent = span_of(pair * 2 + which, share, s)

                def more(step, inner, source=source, count=count):
                    target = pl.ds(count + step * STEP, STEP)
                    stage[target, :] = contrib[pl.ds(source + step * STEP, STEP), :]
                    tags[target, :] = names[pl.ds(source + step * STEP, STEP), :]
                    return inner

                lax.fori_loop(0, (extent + STEP - 1) // STEP, more, 0)
                count = count + extent
            total[...] = jnp.zeros_like(total)

            def add(start, extent, value):
                total[:, pl.ds(start, extent)] += value

            def chunk(at, inner, count=count):
                place = pl.ds(pl.multiple_of(at * DEPTH, DEPTH), DEPTH)
                product(stage[place, :], tags[place, :], at * DEPTH, count, add)
                return inner

            lax.fori_loop(0, (count + DEPTH - 1) // DEPTH, chunk, 0)
            ready[spot(slot, which, share, 0, WIDTH)] = total[...].astype(jnp.bfloat16)

    def one_pair(pair, slot, found, here, there):
        @pl.when(pair >= 2)
        def _():
            for which in range(2):
                for half in range(ratio):
                    put(pair - 2, slot, which, half).wait()

        later = merge(jnp.minimum(pair + 1, windows // 2 - 1), *there)
        for which in range(2):
            for share in range(shares):
                at = which * shares + share

                def store(start, extent, value, which=which, share=share):
                    ready[spot(slot, which, share, start, extent)] = value.astype(jnp.bfloat16)

                product(here[0][at, pl.ds(0, DEPTH), :], here[1][at, pl.ds(0, DEPTH), :], 0, found[at], store)
        for which in range(2):

            @pl.when(found[2 * shares + which] > 0)
            def _():
                slow(pair, slot, which)

            for half in range(ratio):
                put(pair, slot, which, half).start()
        return later

    a, b = (stage_a, tags_a), (stage_b, tags_b)

    def two_pairs(step, found):
        found = one_pair(step * 2, 0, found, a, b)
        return one_pair(step * 2 + 1, 1, found, b, a)

    lax.fori_loop(0, windows // 4, two_pairs, merge(jnp.int32(0), *a))
    for slot in range(2):
        for which in range(2):
            for half in range(ratio):
                put(jnp.int32(windows // 2 - 2 + slot), slot, which, half).wait()


def align(held, rows, ratio, planes, capacity):
    sources, height, length = held.shape
    room = height - META
    deep = -(-(sources * capacity + STEP) // DEPTH) * DEPTH
    shares = ratio * rows // WIDTH
    cfg = (sources, room, rows, ratio, planes)
    short = pltpu.VMEM((2 * shares, DEPTH + STEP, LANES), jnp.float32)
    return pl.pallas_call(
        functools.partial(align_kernel, cfg),
        out_shape=jax.ShapeDtypeStruct((planes, ratio, WINDOWS * length, rows), jnp.bfloat16),
        in_specs=[ANY],
        out_specs=ANY,
        scratch_shapes=[
            pltpu.VMEM((sources * height, length), jnp.bfloat16),
            pltpu.VMEM((2 * sources, LANES), jnp.int32),
            pltpu.SMEM((2 * sources, LANES), jnp.int32),
            pltpu.VMEM((sources * room + STEP, length), jnp.float32),
            pltpu.VMEM((sources * room + STEP, LANES), jnp.float32),
            short,
            short,
            short,
            short,
            pltpu.VMEM((deep, length), jnp.float32),
            pltpu.VMEM((deep, LANES), jnp.float32),
            pltpu.VMEM((length, WIDTH), jnp.float32),
            pltpu.VMEM((2, 2, ratio, length, rows), jnp.bfloat16),
            pltpu.SemaphoreType.DMA((sources + 1,)),
            pltpu.SemaphoreType.DMA((2, 2, ratio)),
        ],
        compiler_params=pltpu.CompilerParams(vmem_limit_bytes=GRANT),
        cost_estimate=pl.CostEstimate(flops=10 * 10**9, bytes_accessed=2 * 10**7, transcendentals=0),
        name="align",
    )(held)


def far_first(planes):
    return [sorted(range(planes), key=lambda p: (-abs(p - z), -p)) for z in range(planes)]


def reduce_kernel(
    cfg, aligned, calib, early, later, out, left, near, far, stage, up, down, kept, total, answer,
    left_sems, near_sems, early_sems, later_sems, far_send, far_recv, up_send, up_recv, down_send, down_recv, out_sems,
):
    planes, ratio, pieces = cfg
    t, c = lax.axis_index("tm"), lax.axis_index("col")
    plane, lot = t // ratio, lax.rem(t, ratio)
    rows = calib.shape[0]
    gap = rows - later.shape[1]
    split = rows // 2
    order = far_first(planes)

    def columns(piece):
        return pl.ds(pl.multiple_of(piece * PIECE, PIECE), PIECE)

    def far_copy(step, piece, part):
        place = pl.ds(0, gap) if part == 2 else pl.ds(part * split, split)
        return pltpu.make_async_remote_copy(
            src_ref=calib.at[place, columns(piece)],
            dst_ref=far.at[step - 1, piece, place],
            send_sem=far_send.at[step - 1, piece, part],
            recv_sem=far_recv.at[step - 1, piece, part],
            device_id=(plane * ratio + lax.rem(lot - step + ratio, ratio), c),
            device_id_type=MESH,
        )

    def target(turn):
        return pick(order, plane, turn)

    def near_load(piece):
        return pltpu.make_async_copy(calib.at[:, columns(piece)], near.at[piece], near_sems.at[piece])

    def early_load(step):
        return pltpu.make_async_copy(
            early.at[step - 1], far.at[step - 1, 0], early_sems.at[step - 1]
        )

    def later_load(step):
        return pltpu.make_async_copy(
            later.at[step - 1], far.at[step - 1, 1, pl.ds(gap, rows - gap)], later_sems.at[step - 1]
        )

    def left_load(turn):
        where = target(turn)
        return pltpu.make_async_copy(aligned.at[where], left.at[where], left_sems.at[turn])

    steps = range(1, ratio)
    opening = [left_load(0), near_load(0)] + [early_load(step) for step in steps]
    for load in opening:
        load.start()
    barrier = pltpu.get_barrier_semaphore()
    peers = [(True, (plane * ratio + lax.rem(lot + step, ratio), c)) for step in steps]
    peers += [(plane > 0, (t - ratio, c)), (plane < planes - 1, (t + ratio, c))]
    for near_by, peer in peers:

        @pl.when(near_by)
        def _():
            pl.semaphore_signal(barrier, inc=1, device_id=peer, device_id_type=MESH)

    pl.semaphore_wait(
        barrier, ratio - 1 + jnp.where(plane > 0, 1, 0) + jnp.where(plane < planes - 1, 1, 0)
    )

    late = [(1, 2)] + [(piece, part) for piece in range(2, pieces) for part in range(2)]
    for piece, part in late:
        for step in steps:
            far_copy(step, piece, part).start()
    for load in opening:
        load.wait()
    for turn in range(1, planes):
        left_load(turn).start()
    for piece in range(1, pieces):
        near_load(piece).start()
    for step in steps:
        later_load(step).start()

    strip = left.shape[2] // STRIPS

    def rows_of(part):
        return pl.ds(pl.multiple_of(part * strip, strip), strip)

    def hop(piece, where, part, buffer, sends, recvs, side):
        return pltpu.make_async_remote_copy(
            src_ref=stage.at[piece, where, rows_of(part)],
            dst_ref=buffer.at[piece, where, rows_of(part)],
            send_sem=sends.at[piece, where, part],
            recv_sem=recvs.at[piece, where, part],
            device_id=(t + side * ratio, c),
            device_id_type=MESH,
        )

    def go_up(piece, where, part):
        return hop(piece, where, part, up, up_send, up_recv, 1)

    def go_down(piece, where, part):
        return hop(piece, where, part, down, down_send, down_recv, -1)

    def one_piece(piece, carry):
        @pl.when(piece > 0)
        def _():
            near_load(piece).wait()

        @pl.when(piece == 1)
        def _():
            for step in steps:
                later_load(step).wait()
                far_copy(step, 1, 2).wait_recv()

        @pl.when(piece > 1)
        def _():
            for step in steps:
                for part in range(2):
                    far_copy(step, piece, part).wait_recv()

        def one_turn(step, inner):
            turn, part = step // STRIPS, lax.rem(step, STRIPS)
            where, here = target(turn), rows_of(part)

            @pl.when((piece == 0) & (turn > 0) & (part == 0))
            def _():
                left_load(turn).wait()

            value = jnp.dot(left[where, 0, here], near[piece], preferred_element_type=jnp.float32)
            for side in range(1, ratio):
                value = value + jnp.dot(
                    left[where, side, here], far[side - 1, piece], preferred_element_type=jnp.float32
                )
            total[...] = value

            @pl.when((where > plane) & (plane > 0))
            def _():
                go_up(piece, where, part).wait_recv()
                stage[piece, where, here] = (total[...] + up[piece, where, here].astype(jnp.float32)).astype(jnp.bfloat16)

            @pl.when((where < plane) & (plane < planes - 1))
            def _():
                go_down(piece, where, part).wait_recv()
                stage[piece, where, here] = (total[...] + down[piece, where, here].astype(jnp.float32)).astype(jnp.bfloat16)

            @pl.when(((where > plane) & (plane == 0)) | ((where < plane) & (plane == planes - 1)))
            def _():
                stage[piece, where, here] = total[...].astype(jnp.bfloat16)

            @pl.when(where > plane)
            def _():
                go_up(piece, where, part).start()

            @pl.when(where < plane)
            def _():
                go_down(piece, where, part).start()

            @pl.when(where == plane)
            def _():
                kept[piece, here] = total[...]

            return inner

        lax.fori_loop(0, planes * STRIPS, one_turn, 0)
        return carry

    lax.fori_loop(0, pieces, one_piece, 0)

    def put(piece):
        return pltpu.make_async_copy(
            answer.at[piece],
            out.at[:, pl.ds(pl.multiple_of(piece * PIECE, PIECE), PIECE)],
            out_sems.at[piece],
        )

    def finish(piece, carry):
        for part in range(STRIPS):
            here = pl.ds(part * strip, strip)

            @pl.when(plane > 0)
            def _():
                go_up(piece, plane, part).wait_recv()
                kept[piece, here] += up[piece, plane, here].astype(jnp.float32)

            @pl.when(plane < planes - 1)
            def _():
                go_down(piece, plane, part).wait_recv()
                kept[piece, here] += down[piece, plane, here].astype(jnp.float32)

        answer[piece] = kept[piece].astype(jnp.bfloat16)
        put(piece).start()
        return carry

    lax.fori_loop(0, pieces, finish, 0)

    def drain(piece, carry):
        put(piece).wait()
        for where in range(planes):
            for part in range(STRIPS):

                @pl.when(where > plane)
                def _():
                    go_up(piece, where, part).wait_send()

                @pl.when(where < plane)
                def _():
                    go_down(piece, where, part).wait_send()

        return carry

    lax.fori_loop(0, pieces, drain, 0)
    for piece, part in late:
        for step in steps:
            far_copy(step, piece, part).wait_send()


def reduce(aligned, calib, early, later):
    planes, ratio, height, rows = aligned.shape
    outputs = calib.shape[1]
    pieces = outputs // PIECE
    cfg = (planes, ratio, pieces)
    far = (ratio - 1, pieces, 3)
    hops = (pieces, planes, STRIPS)
    return pl.pallas_call(
        functools.partial(reduce_kernel, cfg),
        out_shape=jax.ShapeDtypeStruct((height, outputs), jnp.bfloat16),
        in_specs=[ANY] * 4,
        out_specs=ANY,
        scratch_shapes=[
            pltpu.VMEM((planes, ratio, height, rows), jnp.bfloat16),
            pltpu.VMEM((pieces, rows, PIECE), jnp.bfloat16),
            pltpu.VMEM((ratio - 1, pieces, rows, PIECE), jnp.bfloat16),
            pltpu.VMEM((pieces, planes, height, PIECE), jnp.bfloat16),
            pltpu.VMEM((pieces, planes, height, PIECE), jnp.bfloat16),
            pltpu.VMEM((pieces, planes, height, PIECE), jnp.bfloat16),
            pltpu.VMEM((pieces, height, PIECE), jnp.float32),
            pltpu.VMEM((height // STRIPS, PIECE), jnp.float32),
            pltpu.VMEM((pieces, height, PIECE), jnp.bfloat16),
            pltpu.SemaphoreType.DMA((planes,)),
            pltpu.SemaphoreType.DMA((pieces,)),
            pltpu.SemaphoreType.DMA((ratio - 1,)),
            pltpu.SemaphoreType.DMA((ratio - 1,)),
            pltpu.SemaphoreType.DMA(far),
            pltpu.SemaphoreType.DMA(far),
            pltpu.SemaphoreType.DMA(hops),
            pltpu.SemaphoreType.DMA(hops),
            pltpu.SemaphoreType.DMA(hops),
            pltpu.SemaphoreType.DMA(hops),
            pltpu.SemaphoreType.DMA((pieces,)),
        ],
        compiler_params=pltpu.CompilerParams(
            collective_id=1, has_side_effects=True, vmem_limit_bytes=GRANT
        ),
        cost_estimate=pl.CostEstimate(flops=20 * 10**9, bytes_accessed=3 * 10**7, transcendentals=0),
        name="reduce",
    )(aligned, calib, early, later)


def per_device(
    block_values, block_shifts, block_sensor, block_window, block_owner, block_counts, calibration
):
    owners = lax.axis_size("tm")
    cols = lax.axis_size("col")
    ratio = owners // cols
    planes = owners // ratio
    rows, outputs = calibration.shape
    blocks = block_values.shape[1]
    capacity = min(blocks, blocks * 3 // (2 * owners))
    def shifted(step):
        return [((t // ratio) * ratio + (t % ratio + step) % ratio, t) for t in range(owners)]

    by_lane = (blocks // LANES, LANES)
    held, early, part = deliver(
        block_values[0], block_shifts[0], block_sensor.reshape(by_lane), block_window.reshape(by_lane),
        block_owner.reshape(by_lane), block_counts, calibration, owners, cols, capacity,
    )
    later = jnp.stack([lax.ppermute(part, "tm", shifted(step)) for step in range(1, ratio)])
    aligned = align(held, rows, ratio, planes, capacity)
    return reduce(aligned, calibration, early, later)


def solution(mesh):
    placed = (
        P("col", "tm", None),
        P("col", "tm", None),
        P("col", "tm"),
        P("col", "tm"),
        P("col", "tm", None),
        P("col", "tm"),
        P("tm", "col"),
    )
    return jax.shard_map(
        per_device, mesh=mesh, in_specs=placed, out_specs=P("tm", "col"), check_vma=False
    )
```
